32 devices in a mesh: rhs: 1 (over z), mode1: 4 (over y), mode2: 4 (over x), mode3: 2 (over core).
Axes of the slice: x: 4, y: 4, z: 1, core: 2. Of those that a mesh axis runs over, the one named last changes fastest.
The devices are a block of a 4x4x8 slice.
Arguments:
- x_vol: bfloat16 [8, 128, 256, 512], P('rhs', 'mode1', 'mode2', 'mode3')
- diag_vals: float32 [128, 256, 512], P('mode1', 'mode2', 'mode3')
- a_mode1: bfloat16 [128, 128], replicated
- a_mode2: bfloat16 [256, 256], replicated
- a_mode3: bfloat16 [512, 512], replicated
- b_mode1: bfloat16 [128, 128], replicated
- b_mode2: bfloat16 [256, 256], replicated
- b_mode3: bfloat16 [512, 512], replicated
Outputs:
- output: float32 [8, 128, 256, 512], P('rhs', 'mode1', 'mode2', 'mode3')
All inputs are finite; a program needn't handle non-finite values.
Results may differ from the reference program's by a relative error of at most 0.010905.
Values are sent between devices in bfloat16 or wider.
A program may use at most 768 MiB of HBM per device.

```python
import jax
import jax.numpy as jnp
from jax import lax

RHS_COUNT = 8
MODE1_LEN = 128
MODE2_LEN = 256
MODE3_LEN = 512


def factor(sub_key, size):
    return (jax.random.normal(sub_key, (size, size), jnp.float32) * (3.0 * size) ** -0.5).astype(jnp.bfloat16)


def setup_inputs(seed: int = 0, part: int = 0) -> dict:
    base_key = jax.random.key(seed)
    key_list = jax.random.split(base_key, 8)
    own_key = jax.random.fold_in(key_list[0], part)
    x_vol = jax.random.normal(own_key, (RHS_COUNT, MODE1_LEN, MODE2_LEN, MODE3_LEN), jnp.float32).astype(jnp.bfloat16)
    diag_vals = 10.0 ** jax.random.uniform(key_list[1], (MODE1_LEN, MODE2_LEN, MODE3_LEN), jnp.float32, -0.5, 0.5)
    return {
        'x_vol': x_vol,
        'diag_vals': diag_vals,
        'a_mode1': factor(key_list[2], MODE1_LEN),
        'a_mode2': factor(key_list[3], MODE2_LEN),
        'a_mode3': factor(key_list[4], MODE3_LEN),
        'b_mode1': factor(key_list[5], MODE1_LEN),
        'b_mode2': factor(key_list[6], MODE2_LEN),
        'b_mode3': factor(key_list[7], MODE3_LEN),
    }


def mode_sum(volume, mat_one, mat_two, mat_three):
    volume_f = volume.astype(jnp.float32)
    term_one = jnp.einsum('ia,ajk->ijk', mat_one.astype(jnp.float32), volume_f).astype(jnp.bfloat16)
    term_two = jnp.einsum('jb,ibk->ijk', mat_two.astype(jnp.float32), volume_f).astype(jnp.bfloat16)
    term_three = jnp.einsum('ijc,kc->ijk', volume_f, mat_three.astype(jnp.float32)).astype(jnp.bfloat16)
    return term_one.astype(jnp.float32) + term_two.astype(jnp.float32) + term_three.astype(jnp.float32)


def reference(x_vol, diag_vals, a_mode1, a_mode2, a_mode3, b_mode1, b_mode2, b_mode3):
    def apply_one(volume):
        u_vol = mode_sum(volume, a_mode1, a_mode2, a_mode3).astype(jnp.bfloat16)
        w_vol = (diag_vals * u_vol.astype(jnp.float32)).astype(jnp.bfloat16)
        return mode_sum(w_vol, b_mode1, b_mode2, b_mode3)
    return lax.map(apply_one, x_vol)
```

```python
import functools

import jax
import jax.numpy as jnp
from jax import lax
from jax.experimental import pallas as pl
from jax.experimental.pallas import tpu as pltpu
from jax.sharding import PartitionSpec as P

BF16, F32 = jnp.bfloat16, jnp.float32
AHEAD = 3
SLOTS = 2


def kernel(n1, n2, x, d, a1, a2, a3, b1, b2, b3, z, w, ly, lx, lc, ty, tx,
           f1, f2, g, dv, perm, buf_y, buf_x, mid_a, mid_b, out_y, out_x, vb, cb, yb, xb, ws, zs,
           in_send, in_recv, out_send, out_recv, own_sem, ld):
    rhs, len_i, len_j, len_k = x.shape
    blk_j, blk_i = len_j // n1, len_i // n2
    me_y, me_x, me_c = lax.axis_index('mode1'), lax.axis_index('mode2'), lax.axis_index('mode3')
    other = 1 - me_c
    order_y = [o for o in (1, n1 - 1, *range(2, n1 - 1))]
    order_x = [o for o in (1, n2 - 1, *range(2, n2 - 1))]

    def peer_y(o):
        return lax.rem(me_y + o, n1)

    def peer_x(o):
        return lax.rem(me_x + o, n2)

    def al(v, m):
        return pl.multiple_of(v * m, m)

    def remote(src, dst, send, recv, axis, index):
        return pltpu.make_async_remote_copy(src_ref=src, dst_ref=dst, send_sem=send, recv_sem=recv,
                                            device_id={axis: index}, device_id_type=pl.DeviceIdType.MESH)

    def in_copies(s, v, r):
        y_list, x_list = [], []
        for o in order_y:
            q = peer_y(o)
            y_list.append(remote(v.at[r, :, pl.ds(al(q, blk_j), blk_j), :], ly.at[s, r, pl.ds(al(me_y, len_i), len_i)],
                                 in_send.at[s, r, o - 1], in_recv.at[s, r, o - 1], 'mode1', q))
        for o in order_x:
            p = peer_x(o)
            x_list.append(remote(v.at[r, pl.ds(al(p, blk_i), blk_i)], lx.at[s, r, :, pl.ds(al(me_x, len_j), len_j), :],
                                 in_send.at[s, r, n1 + o - 2], in_recv.at[s, r, n1 + o - 2], 'mode2', p))
        core = remote(v.at[r], lc.at[s, r], in_send.at[s, r, n1 + n2 - 2], in_recv.at[s, r, n1 + n2 - 2], 'mode3', other)
        return y_list, x_list, core

    def send_in(s, v, r):
        y_list, x_list, core = in_copies(s, v, r)
        for pair in zip(x_list, y_list):
            for copy in pair:
                copy.start()
        core.start()

    def out_x_copies(s, r, slot):
        copies = []
        for o in order_x:
            p = peer_x(o)
            copies.append(remote(out_x.at[s, slot, :, pl.ds(al(p, len_j), len_j), :], tx.at[s, r, pl.ds(al(me_x, blk_i), blk_i)],
                                 out_send.at[s, r, n1 + o - 2], out_recv.at[s, r, n1 + o - 2], 'mode2', p))
        own = pltpu.make_async_copy(out_x.at[s, slot, :, pl.ds(al(me_x, len_j), len_j), :],
                                    tx.at[s, r, pl.ds(al(me_x, blk_i), blk_i)], own_sem.at[s, slot, 1])
        return copies, own

    def out_y_copies(s, r, slot):
        copies = []
        for o in order_y:
            q = peer_y(o)
            copies.append(remote(out_y.at[s, slot, pl.ds(al(q, len_i), len_i)], ty.at[s, r, :, pl.ds(al(me_y, blk_j), blk_j), :],
                                 out_send.at[s, r, o - 1], out_recv.at[s, r, o - 1], 'mode1', q))
        own = pltpu.make_async_copy(out_y.at[s, slot, pl.ds(al(me_y, len_i), len_i)],
                                    ty.at[s, r, :, pl.ds(al(me_y, blk_j), blk_j), :], own_sem.at[s, slot, 0])
        return copies, own

    def products(s, v, r):
        slot = lax.rem(r, SLOTS)
        y_list, x_list, _ = in_copies(s, v, r)
        for copy in x_list + y_list:
            copy.wait_send()
            copy.wait_recv()
        loads = []
        for o in range(n2):
            p = peer_x(o)
            src = v.at[r, pl.ds(al(me_x, blk_i), blk_i)] if o == 0 else lx.at[s, r, :, pl.ds(al(p, len_j), len_j), :]
            loads.append(pltpu.make_async_copy(src, buf_x.at[:, pl.ds(al(p, len_j), len_j), :], ld.at[n1 + o]))
        for o in range(n1):
            q = peer_y(o)
            src = v.at[r, :, pl.ds(al(me_y, blk_j), blk_j), :] if o == 0 else ly.at[s, r, pl.ds(al(q, len_i), len_i)]
            loads.append(pltpu.make_async_copy(src, buf_y.at[pl.ds(al(q, len_i), len_i)], ld.at[o]))
        for copy in loads:
            copy.start()
        for copy in loads[:n2]:
            copy.wait()

        @pl.loop(0, blk_i)
        def _(i):
            out_x[s, slot, i] = jnp.dot(f2[s], buf_x[i], preferred_element_type=F32).astype(BF16)

        copies, own = out_x_copies(s, r, slot)
        for copy in copies + [own]:
            copy.start()
        for copy in loads[n2:]:
            copy.wait()

        blocks = buf_y.shape[0] // blk_j

        @pl.loop(0, blocks)
        def _(b):
            rows = pl.ds(al(b, blk_j), blk_j)
            block = buf_y[rows].reshape(blk_j * blk_j, len_k)
            mid_a[:, rows, :] = jnp.dot(perm[...], block, preferred_element_type=F32).astype(BF16).reshape(blk_j, blk_j, len_k)

        @pl.loop(0, blk_j)
        def _(j):
            mid_b[j] = jnp.dot(f1[s], mid_a[j], preferred_element_type=F32).astype(BF16)

        @pl.loop(0, blocks)
        def _(b):
            rows = pl.ds(al(b, blk_j), blk_j)
            block = mid_b[:, rows, :].reshape(blk_j * blk_j, len_k)
            out_y[s, slot, rows] = jnp.dot(perm[...], block, preferred_element_type=F32).astype(BF16).reshape(blk_j, blk_j, len_k)

        copies, own = out_y_copies(s, r, slot)
        for copy in copies + [own]:
            copy.start()

    def combine(s, v, r):
        slot = lax.rem(r, SLOTS)
        core = in_copies(s, v, r)[2]
        core.wait_send()
        core.wait_recv()
        copies_x, own_x = out_x_copies(s, r, slot)
        copies_y, own_y = out_y_copies(s, r, slot)
        for copy in copies_x + copies_y:
            copy.wait_send()
            copy.wait_recv()
        own_x.wait()
        own_y.wait()
        loads = [pltpu.make_async_copy(src, dst, ld.at[n]) for n, (src, dst) in enumerate(
            ((v.at[r], vb), (lc.at[s, r], cb), (ty.at[s, r], yb), (tx.at[s, r], xb)))]
        for copy in loads:
            copy.start()
        for copy in loads:
            copy.wait()
        step = max(1, 256 // len_j)
        flat = (step * len_j, len_k)

        @pl.loop(0, len_i // step)
        def _(b):
            rows = pl.ds(b * step, step)
            third = (jnp.dot(vb[rows].reshape(flat), g[s, 0], preferred_element_type=F32)
                     + jnp.dot(cb[rows].reshape(flat), g[s, 1], preferred_element_type=F32)).astype(BF16)
            total = (yb[rows].reshape(flat).astype(F32) + xb[rows].reshape(flat).astype(F32)) + third.astype(F32)
            if s == 0:
                scaled = dv[rows].reshape(flat) * total.astype(BF16).astype(F32)
                ws[rows] = scaled.astype(BF16).reshape(step, len_j, len_k)
            else:
                zs[rows] = total.reshape(step, len_j, len_k)

        store = pltpu.make_async_copy(ws, w.at[r], ld.at[0]) if s == 0 else pltpu.make_async_copy(zs, z.at[r], ld.at[0])
        store.start()
        store.wait()

    barrier = pltpu.get_barrier_semaphore()
    for o in range(1, n1):
        pl.semaphore_signal(barrier, inc=1, device_id={'mode1': peer_y(o)}, device_id_type=pl.DeviceIdType.MESH)
    for o in range(1, n2):
        pl.semaphore_signal(barrier, inc=1, device_id={'mode2': peer_x(o)}, device_id_type=pl.DeviceIdType.MESH)
    pl.semaphore_signal(barrier, inc=1, device_id={'mode3': other}, device_id_type=pl.DeviceIdType.MESH)
    pl.semaphore_wait(barrier, n1 + n2 - 1)

    for r in range(AHEAD):
        send_in(0, x, r)

    mine, theirs = pl.ds(al(me_c, len_k), len_k), pl.ds(al(other, len_k), len_k)
    loads = [pltpu.make_async_copy(src, dst, ld.at[n]) for n, (src, dst) in enumerate((
        (a1, f1.at[0]), (b1, f1.at[1]), (a2, f2.at[0]), (b2, f2.at[1]), (d, dv),
        (a3.at[mine, mine], g.at[0, 0]), (a3.at[mine, theirs], g.at[0, 1]),
        (b3.at[mine, mine], g.at[1, 0]), (b3.at[mine, theirs], g.at[1, 1])))]
    for copy in loads:
        copy.start()
    size = blk_j * blk_j
    row = lax.broadcasted_iota(jnp.int32, (size, size), 0)
    col = lax.broadcasted_iota(jnp.int32, (size, size), 1)
    perm[...] = jnp.where(col == lax.rem(row, blk_j) * blk_j + row // blk_j, 1.0, 0.0).astype(BF16)
    for copy in loads:
        copy.wait()
    for s in range(2):
        for c in range(2):
            g[s, c] = g[s, c].astype(F32).T.astype(BF16)

    @pl.loop(0, rhs + 3)
    def _(n):
        @pl.when(n < rhs)
        def _():
            products(0, x, n)

        @pl.when(n + AHEAD < rhs)
        def _():
            send_in(0, x, n + AHEAD)

        @pl.when((n >= 1) & (n < rhs + 1))
        def _():
            combine(0, x, n - 1)
            send_in(1, w, n - 1)

        @pl.when((n >= 2) & (n < rhs + 2))
        def _():
            products(1, w, n - 2)

        @pl.when(n >= 3)
        def _():
            combine(1, w, n - 3)


def solution(mesh):
    n1, n2, n3 = mesh.shape['mode1'], mesh.shape['mode2'], mesh.shape['mode3']
    vol_spec = P('rhs', 'mode1', 'mode2', 'mode3')
    diag_spec = P('mode1', 'mode2', 'mode3')

    def local_op(x_vol, diag_vals, a1, a2, a3, b1, b2, b3):
        rhs, len_i, len_j, len_k = x_vol.shape
        m1, m2 = len_i * n1, len_j * n2
        blk_j, blk_i = len_j // n1, len_i // n2
        any_spec = pl.BlockSpec(memory_space=pl.ANY)
        outs = [
            jax.ShapeDtypeStruct((rhs, len_i, len_j, len_k), F32),
            jax.ShapeDtypeStruct((rhs, len_i, len_j, len_k), BF16),
            jax.ShapeDtypeStruct((2, rhs, m1, blk_j, len_k), BF16),
            jax.ShapeDtypeStruct((2, rhs, blk_i, m2, len_k), BF16),
            jax.ShapeDtypeStruct((2, rhs, len_i, len_j, len_k), BF16),
            jax.ShapeDtypeStruct((2, rhs, len_i, len_j, len_k), BF16),
            jax.ShapeDtypeStruct((2, rhs, len_i, len_j, len_k), BF16),
        ]
        vmem, dma = pltpu.VMEM, pltpu.SemaphoreType.DMA
        local = (len_i, len_j, len_k)
        return pl.pallas_call(
            functools.partial(kernel, n1, n2),
            out_shape=outs,
            in_specs=[any_spec] * 8,
            out_specs=[any_spec] * len(outs),
            scratch_shapes=[
                vmem((2, m1, m1), BF16), vmem((2, m2, m2), BF16), vmem((2, 2, len_k, len_k), BF16), vmem(local, F32),
                vmem((blk_j * blk_j, blk_j * blk_j), BF16),
                vmem((m1, blk_j, len_k), BF16), vmem((blk_i, m2, len_k), BF16),
                vmem((blk_j, m1, len_k), BF16), vmem((blk_j, m1, len_k), BF16),
                vmem((2, SLOTS, m1, blk_j, len_k), BF16), vmem((2, SLOTS, blk_i, m2, len_k), BF16),
                vmem(local, BF16), vmem(local, BF16), vmem(local, BF16), vmem(local, BF16),
                vmem(local, BF16), vmem(local, F32),
                dma((2, rhs, n1 + n2 - 1)), dma((2, rhs, n1 + n2 - 1)),
                dma((2, rhs, n1 + n2 - 2)), dma((2, rhs, n1 + n2 - 2)),
                dma((2, SLOTS, 2)), dma((12,)),
            ],
            compiler_params=pltpu.CompilerParams(collective_id=0, has_side_effects=True, vmem_limit_bytes=60 * 1024 * 1024),
            name='kron',
        )(x_vol, diag_vals, a1, a2, a3, b1, b2, b3)[0]

    return jax.shard_map(local_op, mesh=mesh, in_specs=(vol_spec, diag_spec, P(), P(), P(), P(), P(), P()), out_specs=vol_spec, check_vma=False)
```

```python
import functools

import jax
import jax.numpy as jnp
from jax import lax
from jax.experimental import pallas as pl
from jax.experimental.pallas import tpu as pltpu
from jax.sharding import PartitionSpec as P

BF16, F32 = jnp.bfloat16, jnp.float32
AHEAD = 3
SLOTS = 2


def kernel(n1, n2, x, d, a1, a2, a3, b1, b2, b3, z, third_last, w, ly, lx, lc, ty, tx,
           f1, f2, g, dv, perm, buf_y, buf_x, mid_a, mid_b, out_y, out_x, vb, cb, yb, xb, ws,
           in_send, in_recv, out_send, out_recv, own_sem, ld):
    rhs, len_i, len_j, len_k = x.shape
    blk_j, blk_i = len_j // n1, len_i // n2
    me_y, me_x, me_c = lax.axis_index('mode1'), lax.axis_index('mode2'), lax.axis_index('mode3')
    other = 1 - me_c
    order_y = [o for o in (1, n1 - 1, *range(2, n1 - 1))]
    order_x = [o for o in (1, n2 - 1, *range(2, n2 - 1))]

    def peer_y(o):
        return lax.rem(me_y + o, n1)

    def peer_x(o):
        return lax.rem(me_x + o, n2)

    def al(v, m):
        return pl.multiple_of(v * m, m)

    def remote(src, dst, send, recv, axis, index):
        return pltpu.make_async_remote_copy(src_ref=src, dst_ref=dst, send_sem=send, recv_sem=recv,
                                            device_id={axis: index}, device_id_type=pl.DeviceIdType.MESH)

    def in_copies(s, v, r):
        y_list, x_list = [], []
        for o in order_y:
            q = peer_y(o)
            y_list.append(remote(v.at[r, :, pl.ds(al(q, blk_j), blk_j), :], ly.at[s, r, pl.ds(al(me_y, len_i), len_i)],
                                 in_send.at[s, r, o - 1], in_recv.at[s, r, o - 1], 'mode1', q))
        for o in order_x:
            p = peer_x(o)
            x_list.append(remote(v.at[r, pl.ds(al(p, blk_i), blk_i)], lx.at[s, r, :, pl.ds(al(me_x, len_j), len_j), :],
                                 in_send.at[s, r, n1 + o - 2], in_recv.at[s, r, n1 + o - 2], 'mode2', p))
        core = remote(v.at[r], lc.at[s, r], in_send.at[s, r, n1 + n2 - 2], in_recv.at[s, r, n1 + n2 - 2], 'mode3', other)
        return y_list, x_list, core

    def send_in(s, v, r):
        y_list, x_list, core = in_copies(s, v, r)
        for pair in zip(x_list, y_list):
            for copy in pair:
                copy.start()
        core.start()

    def out_x_copies(s, r, slot):
        copies = []
        for o in order_x:
            p = peer_x(o)
            copies.append(remote(out_x.at[s, slot, :, pl.ds(al(p, len_j), len_j), :], tx.at[s, r, pl.ds(al(me_x, blk_i), blk_i)],
                                 out_send.at[s, r, n1 + o - 2], out_recv.at[s, r, n1 + o - 2], 'mode2', p))
        own = pltpu.make_async_copy(out_x.at[s, slot, :, pl.ds(al(me_x, len_j), len_j), :],
                                    tx.at[s, r, pl.ds(al(me_x, blk_i), blk_i)], own_sem.at[s, slot, 1])
        return copies, own

    def out_y_copies(s, r, slot):
        copies = []
        for o in order_y:
            q = peer_y(o)
            copies.append(remote(out_y.at[s, slot, pl.ds(al(q, len_i), len_i)], ty.at[s, r, :, pl.ds(al(me_y, blk_j), blk_j), :],
                                 out_send.at[s, r, o - 1], out_recv.at[s, r, o - 1], 'mode1', q))
        own = pltpu.make_async_copy(out_y.at[s, slot, pl.ds(al(me_y, len_i), len_i)],
                                    ty.at[s, r, :, pl.ds(al(me_y, blk_j), blk_j), :], own_sem.at[s, slot, 0])
        return copies, own

    def products(s, v, r):
        slot = lax.rem(r, SLOTS)
        y_list, x_list, _ = in_copies(s, v, r)
        for copy in x_list + y_list:
            copy.wait_send()
            copy.wait_recv()
        loads = []
        for o in range(n2):
            p = peer_x(o)
            src = v.at[r, pl.ds(al(me_x, blk_i), blk_i)] if o == 0 else lx.at[s, r, :, pl.ds(al(p, len_j), len_j), :]
            loads.append(pltpu.make_async_copy(src, buf_x.at[:, pl.ds(al(p, len_j), len_j), :], ld.at[n1 + o]))
        for o in range(n1):
            q = peer_y(o)
            src = v.at[r, :, pl.ds(al(me_y, blk_j), blk_j), :] if o == 0 else ly.at[s, r, pl.ds(al(q, len_i), len_i)]
            loads.append(pltpu.make_async_copy(src, buf_y.at[pl.ds(al(q, len_i), len_i)], ld.at[o]))
        for copy in loads:
            copy.start()
        for copy in loads[:n2]:
            copy.wait()

        @pl.loop(0, blk_i)
        def _(i):
            out_x[s, slot, i] = jnp.dot(f2[s], buf_x[i], preferred_element_type=F32).astype(BF16)

        copies, own = out_x_copies(s, r, slot)
        for copy in copies + [own]:
            copy.start()
        for copy in loads[n2:]:
            copy.wait()

        blocks = buf_y.shape[0] // blk_j

        @pl.loop(0, blocks)
        def _(b):
            rows = pl.ds(al(b, blk_j), blk_j)
            block = buf_y[rows].reshape(blk_j * blk_j, len_k)
            mid_a[:, rows, :] = jnp.dot(perm[...], block, preferred_element_type=F32).astype(BF16).reshape(blk_j, blk_j, len_k)

        @pl.loop(0, blk_j)
        def _(j):
            mid_b[j] = jnp.dot(f1[s], mid_a[j], preferred_element_type=F32).astype(BF16)

        @pl.loop(0, blocks)
        def _(b):
            rows = pl.ds(al(b, blk_j), blk_j)
            block = mid_b[:, rows, :].reshape(blk_j * blk_j, len_k)
            out_y[s, slot, rows] = jnp.dot(perm[...], block, preferred_element_type=F32).astype(BF16).reshape(blk_j, blk_j, len_k)

        copies, own = out_y_copies(s, r, slot)
        for copy in copies + [own]:
            copy.start()

    step = max(1, 256 // len_j)
    flat = (step * len_j, len_k)

    def wait_core(s, v, r):
        core = in_copies(s, v, r)[2]
        core.wait_send()
        core.wait_recv()

    def wait_out(s, r):
        slot = lax.rem(r, SLOTS)
        copies_x, own_x = out_x_copies(s, r, slot)
        copies_y, own_y = out_y_copies(s, r, slot)
        for copy in copies_x + copies_y:
            copy.wait_send()
            copy.wait_recv()
        own_x.wait()
        own_y.wait()

    def mode3(s, rows):
        return (jnp.dot(vb[rows].reshape(flat), g[s, 0], preferred_element_type=F32)
                + jnp.dot(cb[rows].reshape(flat), g[s, 1], preferred_element_type=F32)).astype(BF16)

    def combine(s, v, r):
        wait_core(s, v, r)
        wait_out(s, r)
        loads = [pltpu.make_async_copy(src, dst, ld.at[n]) for n, (src, dst) in enumerate(
            ((v.at[r], vb), (lc.at[s, r], cb), (ty.at[s, r], yb), (tx.at[s, r], xb)))]
        for copy in loads:
            copy.start()
        for copy in loads:
            copy.wait()

        @pl.loop(0, len_i // step)
        def _(b):
            rows = pl.ds(b * step, step)
            total = (yb[rows].reshape(flat).astype(F32) + xb[rows].reshape(flat).astype(F32)) + mode3(s, rows).astype(F32)
            if s == 0:
                scaled = dv[rows].reshape(flat) * total.astype(BF16).astype(F32)
                ws[rows] = scaled.astype(BF16).reshape(step, len_j, len_k)
            else:
                z[r, rows] = total.reshape(step, len_j, len_k)

        if s == 0:
            store = pltpu.make_async_copy(ws, w.at[r], ld.at[0])
            store.start()
            store.wait()

    barrier = pltpu.get_barrier_semaphore()
    for o in range(1, n1):
        pl.semaphore_signal(barrier, inc=1, device_id={'mode1': peer_y(o)}, device_id_type=pl.DeviceIdType.MESH)
    for o in range(1, n2):
        pl.semaphore_signal(barrier, inc=1, device_id={'mode2': peer_x(o)}, device_id_type=pl.DeviceIdType.MESH)
    pl.semaphore_signal(barrier, inc=1, device_id={'mode3': other}, device_id_type=pl.DeviceIdType.MESH)
    pl.semaphore_wait(barrier, n1 + n2 - 1)

    for r in range(AHEAD):
        send_in(0, x, r)

    mine, theirs = pl.ds(al(me_c, len_k), len_k), pl.ds(al(other, len_k), len_k)
    loads = [pltpu.make_async_copy(src, dst, ld.at[n]) for n, (src, dst) in enumerate((
        (a1, f1.at[0]), (b1, f1.at[1]), (a2, f2.at[0]), (b2, f2.at[1]), (d, dv),
        (a3.at[mine, mine], g.at[0, 0]), (a3.at[mine, theirs], g.at[0, 1]),
        (b3.at[mine, mine], g.at[1, 0]), (b3.at[mine, theirs], g.at[1, 1])))]
    for copy in loads:
        copy.start()
    size = blk_j * blk_j
    row = lax.broadcasted_iota(jnp.int32, (size, size), 0)
    col = lax.broadcasted_iota(jnp.int32, (size, size), 1)
    perm[...] = jnp.where(col == lax.rem(row, blk_j) * blk_j + row // blk_j, 1.0, 0.0).astype(BF16)
    for copy in loads:
        copy.wait()
    for s in range(2):
        for c in range(2):
            g[s, c] = g[s, c].astype(F32).T.astype(BF16)

    @pl.loop(0, rhs + 2)
    def _(n):
        @pl.when(n < rhs)
        def _():
            products(0, x, n)

        @pl.when(n + AHEAD < rhs)
        def _():
            send_in(0, x, n + AHEAD)

        @pl.when((n >= 1) & (n < rhs + 1))
        def _():
            combine(0, x, n - 1)
            send_in(1, w, n - 1)

        @pl.when((n >= 2) & (n < rhs + 2))
        def _():
            products(1, w, n - 2)

        @pl.when((n >= 3) & (n < rhs + 2))
        def _():
            combine(1, w, n - 3)

    last = rhs - 1
    wait_core(1, w, last)
    loads = [pltpu.make_async_copy(w.at[last], vb, ld.at[0]), pltpu.make_async_copy(lc.at[1, last], cb, ld.at[1])]
    for copy in loads:
        copy.start()
    for copy in loads:
        copy.wait()

    @pl.loop(0, len_i // step)
    def _(b):
        rows = pl.ds(b * step, step)
        third_last[rows] = mode3(1, rows).reshape(step, len_j, len_k)

    wait_out(1, last)


def finish(z_first, third, ty, tx, z, yb, xb, zb, sem):
    done, len_i = z_first.shape[0], z_first.shape[1]
    loads = [pltpu.make_async_copy(ty.at[1, done], yb, sem.at[done]), pltpu.make_async_copy(tx.at[1, done], xb, sem.at[done + 1])]
    for copy in loads:
        copy.start()
    writes = [pltpu.make_async_copy(z_first.at[r], z.at[r], sem.at[r]) for r in range(done)]
    for copy in writes:
        copy.start()
    for copy in loads:
        copy.wait()

    @pl.loop(0, len_i)
    def _(i):
        zb[i] = (yb[i].astype(F32) + xb[i].astype(F32)) + third[i].astype(F32)

    writes.append(pltpu.make_async_copy(zb, z.at[done], sem.at[done]))
    writes[-1].start()
    for copy in writes:
        copy.wait()


def solution(mesh):
    n1, n2, n3 = mesh.shape['mode1'], mesh.shape['mode2'], mesh.shape['mode3']
    vol_spec = P('rhs', 'mode1', 'mode2', 'mode3')
    diag_spec = P('mode1', 'mode2', 'mode3')

    def local_op(x_vol, diag_vals, a1, a2, a3, b1, b2, b3):
        rhs, len_i, len_j, len_k = x_vol.shape
        m1, m2 = len_i * n1, len_j * n2
        blk_j, blk_i = len_j // n1, len_i // n2
        any_spec = pl.BlockSpec(memory_space=pl.ANY)
        vmem_spec = pl.BlockSpec(memory_space=pltpu.VMEM)
        outs = [
            pltpu.VMEM((rhs - 1, len_i, len_j, len_k), F32),
            pltpu.VMEM((len_i, len_j, len_k), BF16),
            jax.ShapeDtypeStruct((rhs, len_i, len_j, len_k), BF16),
            jax.ShapeDtypeStruct((2, rhs, m1, blk_j, len_k), BF16),
            jax.ShapeDtypeStruct((2, rhs, blk_i, m2, len_k), BF16),
            jax.ShapeDtypeStruct((2, rhs, len_i, len_j, len_k), BF16),
            jax.ShapeDtypeStruct((2, rhs, len_i, len_j, len_k), BF16),
            jax.ShapeDtypeStruct((2, rhs, len_i, len_j, len_k), BF16),
        ]
        vmem, dma = pltpu.VMEM, pltpu.SemaphoreType.DMA
        local = (len_i, len_j, len_k)
        res = pl.pallas_call(
            functools.partial(kernel, n1, n2),
            out_shape=outs,
            in_specs=[any_spec] * 8,
            out_specs=[vmem_spec] * 2 + [any_spec] * (len(outs) - 2),
            scratch_shapes=[
                vmem((2, m1, m1), BF16), vmem((2, m2, m2), BF16), vmem((2, 2, len_k, len_k), BF16), vmem(local, F32),
                vmem((blk_j * blk_j, blk_j * blk_j), BF16),
                vmem((m1, blk_j, len_k), BF16), vmem((blk_i, m2, len_k), BF16),
                vmem((blk_j, m1, len_k), BF16), vmem((blk_j, m1, len_k), BF16),
                vmem((2, SLOTS, m1, blk_j, len_k), BF16), vmem((2, SLOTS, blk_i, m2, len_k), BF16),
                vmem(local, BF16), vmem(local, BF16), vmem(local, BF16), vmem(local, BF16),
                vmem(local, BF16),
                dma((2, rhs, n1 + n2 - 1)), dma((2, rhs, n1 + n2 - 1)),
                dma((2, rhs, n1 + n2 - 2)), dma((2, rhs, n1 + n2 - 2)),
                dma((2, SLOTS, 2)), dma((12,)),
            ],
            compiler_params=pltpu.CompilerParams(collective_id=0, has_side_effects=True, vmem_limit_bytes=48 * 1024 * 1024),
            name='kron',
        )(x_vol, diag_vals, a1, a2, a3, b1, b2, b3)
        return pl.pallas_call(
            finish,
            out_shape=jax.ShapeDtypeStruct(x_vol.shape, F32),
            in_specs=[vmem_spec] * 2 + [any_spec] * 2,
            out_specs=any_spec,
            scratch_shapes=[vmem(local, BF16), vmem(local, BF16), vmem(local, F32), dma((rhs + 1,))],
            compiler_params=pltpu.CompilerParams(vmem_limit_bytes=48 * 1024 * 1024),
            name='finish',
        )(res[0], res[1], res[-2], res[-1])

    return jax.shard_map(local_op, mesh=mesh, in_specs=(vol_spec, diag_spec, P(), P(), P(), P(), P(), P()), out_specs=vol_spec, check_vma=False)
```

```python
import functools

import jax
import jax.numpy as jnp
from jax import lax
from jax.experimental import pallas as pl
from jax.experimental.pallas import tpu as pltpu
from jax.sharding import PartitionSpec as P

BF16, F32 = jnp.bfloat16, jnp.float32
AHEAD = 3
SLOTS = 2


def kernel(n1, n2, x, d, a1, a2, a3, b1, b2, b3, z, third_last, ty_last, tx_last, w, ly, lx, lc, ty, tx,
           f1, f2, g, dv, perm, buf_y, buf_x, mid_a, mid_b, out_y, out_x, vb, cb, yb, xb, ws,
           in_send, in_recv, out_send, out_recv, own_sem, ld):
    rhs, len_i, len_j, len_k = x.shape
    blk_j, blk_i = len_j // n1, len_i // n2
    me_y, me_x, me_c = lax.axis_index('mode1'), lax.axis_index('mode2'), lax.axis_index('mode3')
    other = 1 - me_c
    order_y = [o for o in (1, n1 - 1, *range(2, n1 - 1))]
    order_x = [o for o in (1, n2 - 1, *range(2, n2 - 1))]

    def peer_y(o):
        return lax.rem(me_y + o, n1)

    def peer_x(o):
        return lax.rem(me_x + o, n2)

    def al(v, m):
        return pl.multiple_of(v * m, m)

    def remote(src, dst, send, recv, axis, index):
        return pltpu.make_async_remote_copy(src_ref=src, dst_ref=dst, send_sem=send, recv_sem=recv,
                                            device_id={axis: index}, device_id_type=pl.DeviceIdType.MESH)

    def in_copies(s, v, r):
        y_list, x_list = [], []
        for o in order_y:
            q = peer_y(o)
            y_list.append(remote(v.at[r, :, pl.ds(al(q, blk_j), blk_j), :], ly.at[s, r, pl.ds(al(me_y, len_i), len_i)],
                                 in_send.at[s, r, o - 1], in_recv.at[s, r, o - 1], 'mode1', q))
        for o in order_x:
            p = peer_x(o)
            x_list.append(remote(v.at[r, pl.ds(al(p, blk_i), blk_i)], lx.at[s, r, :, pl.ds(al(me_x, len_j), len_j), :],
                                 in_send.at[s, r, n1 + o - 2], in_recv.at[s, r, n1 + o - 2], 'mode2', p))
        core = remote(v.at[r], lc.at[s, r], in_send.at[s, r, n1 + n2 - 2], in_recv.at[s, r, n1 + n2 - 2], 'mode3', other)
        return y_list, x_list, core

    def send_in(s, v, r):
        y_list, x_list, core = in_copies(s, v, r)
        for pair in zip(x_list, y_list):
            for copy in pair:
                copy.start()
        core.start()

    def out_x_copies(s, r, slot, last=False):
        copies = []
        home = tx_last if last else tx.at[s, r]
        for o in order_x:
            p = peer_x(o)
            copies.append(remote(out_x.at[s, slot, :, pl.ds(al(p, len_j), len_j), :], home.at[pl.ds(al(me_x, blk_i), blk_i)],
                                 out_send.at[s, r, n1 + o - 2], out_recv.at[s, r, n1 + o - 2], 'mode2', p))
        if last:
            return copies, None
        own = pltpu.make_async_copy(out_x.at[s, slot, :, pl.ds(al(me_x, len_j), len_j), :],
                                    home.at[pl.ds(al(me_x, blk_i), blk_i)], own_sem.at[s, slot, 1])
        return copies, own

    def out_y_copies(s, r, slot, last=False):
        copies = []
        home = ty_last if last else ty.at[s, r]
        for o in order_y:
            q = peer_y(o)
            copies.append(remote(out_y.at[s, slot, pl.ds(al(q, len_i), len_i)], home.at[:, pl.ds(al(me_y, blk_j), blk_j), :],
                                 out_send.at[s, r, o - 1], out_recv.at[s, r, o - 1], 'mode1', q))
        if last:
            return copies, None
        own = pltpu.make_async_copy(out_y.at[s, slot, pl.ds(al(me_y, len_i), len_i)],
                                    home.at[:, pl.ds(al(me_y, blk_j), blk_j), :], own_sem.at[s, slot, 0])
        return copies, own

    def products(s, v, r, last=False):
        slot = lax.rem(r, SLOTS)
        y_list, x_list, _ = in_copies(s, v, r)
        for copy in x_list + y_list:
            copy.wait_send()
            copy.wait_recv()
        loads = []
        for o in range(n2):
            p = peer_x(o)
            src = v.at[r, pl.ds(al(me_x, blk_i), blk_i)] if o == 0 else lx.at[s, r, :, pl.ds(al(p, len_j), len_j), :]
            loads.append(pltpu.make_async_copy(src, buf_x.at[:, pl.ds(al(p, len_j), len_j), :], ld.at[n1 + o]))
        for o in range(n1):
            q = peer_y(o)
            src = v.at[r, :, pl.ds(al(me_y, blk_j), blk_j), :] if o == 0 else ly.at[s, r, pl.ds(al(q, len_i), len_i)]
            loads.append(pltpu.make_async_copy(src, buf_y.at[pl.ds(al(q, len_i), len_i)], ld.at[o]))
        for copy in loads:
            copy.start()
        for copy in loads[:n2]:
            copy.wait()

        @pl.loop(0, blk_i)
        def _(i):
            out_x[s, slot, i] = jnp.dot(f2[s], buf_x[i], preferred_element_type=F32).astype(BF16)

        copies, own = out_x_copies(s, r, slot, last)
        for copy in copies if last else copies + [own]:
            copy.start()
        for copy in loads[n2:]:
            copy.wait()

        blocks = buf_y.shape[0] // blk_j

        @pl.loop(0, blocks)
        def _(b):
            rows = pl.ds(al(b, blk_j), blk_j)
            block = buf_y[rows].reshape(blk_j * blk_j, len_k)
            mid_a[:, rows, :] = jnp.dot(perm[...], block, preferred_element_type=F32).astype(BF16).reshape(blk_j, blk_j, len_k)

        @pl.loop(0, blk_j)
        def _(j):
            mid_b[j] = jnp.dot(f1[s], mid_a[j], preferred_element_type=F32).astype(BF16)

        @pl.loop(0, blocks)
        def _(b):
            rows = pl.ds(al(b, blk_j), blk_j)
            block = mid_b[:, rows, :].reshape(blk_j * blk_j, len_k)
            out_y[s, slot, rows] = jnp.dot(perm[...], block, preferred_element_type=F32).astype(BF16).reshape(blk_j, blk_j, len_k)

        copies, own = out_y_copies(s, r, slot, last)
        for copy in copies if last else copies + [own]:
            copy.start()
        if last:
            tx_last[pl.ds(al(me_x, blk_i), blk_i)] = out_x[s, slot, :, pl.ds(al(me_x, len_j), len_j), :]
            ty_last[:, pl.ds(al(me_y, blk_j), blk_j), :] = out_y[s, slot, pl.ds(al(me_y, len_i), len_i)]

    step = max(1, 256 // len_j)
    flat = (step * len_j, len_k)

    def wait_core(s, v, r):
        core = in_copies(s, v, r)[2]
        core.wait_send()
        core.wait_recv()

    def wait_out(s, r, last=False):
        slot = lax.rem(r, SLOTS)
        copies_x, own_x = out_x_copies(s, r, slot, last)
        copies_y, own_y = out_y_copies(s, r, slot, last)
        for copy in copies_x + copies_y:
            copy.wait_send()
            copy.wait_recv()
        if not last:
            own_x.wait()
            own_y.wait()

    def mode3(s, rows):
        return (jnp.dot(vb[rows].reshape(flat), g[s, 0], preferred_element_type=F32)
                + jnp.dot(cb[rows].reshape(flat), g[s, 1], preferred_element_type=F32)).astype(BF16)

    def combine(s, v, r):
        wait_core(s, v, r)
        wait_out(s, r)
        loads = [pltpu.make_async_copy(src, dst, ld.at[n]) for n, (src, dst) in enumerate(
            ((v.at[r], vb), (lc.at[s, r], cb), (ty.at[s, r], yb), (tx.at[s, r], xb)))]
        for copy in loads:
            copy.start()
        for copy in loads:
            copy.wait()

        @pl.loop(0, len_i // step)
        def _(b):
            rows = pl.ds(b * step, step)
            total = (yb[rows].reshape(flat).astype(F32) + xb[rows].reshape(flat).astype(F32)) + mode3(s, rows).astype(F32)
            if s == 0:
                scaled = dv[rows].reshape(flat) * total.astype(BF16).astype(F32)
                ws[rows] = scaled.astype(BF16).reshape(step, len_j, len_k)
            else:
                z[r, rows] = total.reshape(step, len_j, len_k)

        if s == 0:
            store = pltpu.make_async_copy(ws, w.at[r], ld.at[0])
            store.start()
            store.wait()

    barrier = pltpu.get_barrier_semaphore()
    for o in range(1, n1):
        pl.semaphore_signal(barrier, inc=1, device_id={'mode1': peer_y(o)}, device_id_type=pl.DeviceIdType.MESH)
    for o in range(1, n2):
        pl.semaphore_signal(barrier, inc=1, device_id={'mode2': peer_x(o)}, device_id_type=pl.DeviceIdType.MESH)
    pl.semaphore_signal(barrier, inc=1, device_id={'mode3': other}, device_id_type=pl.DeviceIdType.MESH)
    pl.semaphore_wait(barrier, n1 + n2 - 1)

    for r in range(AHEAD):
        send_in(0, x, r)

    mine, theirs = pl.ds(al(me_c, len_k), len_k), pl.ds(al(other, len_k), len_k)
    loads = [pltpu.make_async_copy(src, dst, ld.at[n]) for n, (src, dst) in enumerate((
        (a1, f1.at[0]), (b1, f1.at[1]), (a2, f2.at[0]), (b2, f2.at[1]), (d, dv),
        (a3.at[mine, mine], g.at[0, 0]), (a3.at[mine, theirs], g.at[0, 1]),
        (b3.at[mine, mine], g.at[1, 0]), (b3.at[mine, theirs], g.at[1, 1])))]
    for copy in loads:
        copy.start()
    size = blk_j * blk_j
    row = lax.broadcasted_iota(jnp.int32, (size, size), 0)
    col = lax.broadcasted_iota(jnp.int32, (size, size), 1)
    perm[...] = jnp.where(col == lax.rem(row, blk_j) * blk_j + row // blk_j, 1.0, 0.0).astype(BF16)
    for copy in loads:
        copy.wait()
    for s in range(2):
        for c in range(2):
            g[s, c] = g[s, c].astype(F32).T.astype(BF16)

    @pl.loop(0, rhs + 1)
    def _(n):
        @pl.when(n < rhs)
        def _():
            products(0, x, n)

        @pl.when(n + AHEAD < rhs)
        def _():
            send_in(0, x, n + AHEAD)

        @pl.when(n >= 1)
        def _():
            combine(0, x, n - 1)
            send_in(1, w, n - 1)

        @pl.when(n >= 2)
        def _():
            products(1, w, n - 2)

        @pl.when(n >= 3)
        def _():
            combine(1, w, n - 3)

    last = rhs - 1
    products(1, w, last, True)
    combine(1, w, last - 1)
    wait_core(1, w, last)
    loads = [pltpu.make_async_copy(w.at[last], vb, ld.at[0]), pltpu.make_async_copy(lc.at[1, last], cb, ld.at[1])]
    for copy in loads:
        copy.start()
    for copy in loads:
        copy.wait()

    @pl.loop(0, len_i // step)
    def _(b):
        rows = pl.ds(b * step, step)
        third_last[rows] = mode3(1, rows).reshape(step, len_j, len_k)

    wait_out(1, last, True)


def finish(z_first, third, ty, tx, z, zb, sem):
    done, len_i = z_first.shape[0], z_first.shape[1]
    writes = [pltpu.make_async_copy(z_first.at[r], z.at[r], sem.at[r]) for r in range(done)]
    for copy in writes:
        copy.start()

    @pl.loop(0, len_i)
    def _(i):
        zb[i] = (ty[i].astype(F32) + tx[i].astype(F32)) + third[i].astype(F32)

    writes.append(pltpu.make_async_copy(zb, z.at[done], sem.at[done]))
    writes[-1].start()
    for copy in writes:
        copy.wait()


def solution(mesh):
    n1, n2, n3 = mesh.shape['mode1'], mesh.shape['mode2'], mesh.shape['mode3']
    vol_spec = P('rhs', 'mode1', 'mode2', 'mode3')
    diag_spec = P('mode1', 'mode2', 'mode3')

    def local_op(x_vol, diag_vals, a1, a2, a3, b1, b2, b3):
        rhs, len_i, len_j, len_k = x_vol.shape
        m1, m2 = len_i * n1, len_j * n2
        blk_j, blk_i = len_j // n1, len_i // n2
        any_spec = pl.BlockSpec(memory_space=pl.ANY)
        vmem_spec = pl.BlockSpec(memory_space=pltpu.VMEM)
        outs = [
            pltpu.VMEM((rhs - 1, len_i, len_j, len_k), F32),
            *[pltpu.VMEM((len_i, len_j, len_k), BF16)] * 3,
            jax.ShapeDtypeStruct((rhs, len_i, len_j, len_k), BF16),
            jax.ShapeDtypeStruct((2, rhs, m1, blk_j, len_k), BF16),
            jax.ShapeDtypeStruct((2, rhs, blk_i, m2, len_k), BF16),
            jax.ShapeDtypeStruct((2, rhs, len_i, len_j, len_k), BF16),
            jax.ShapeDtypeStruct((2, rhs, len_i, len_j, len_k), BF16),
            jax.ShapeDtypeStruct((2, rhs, len_i, len_j, len_k), BF16),
        ]
        vmem, dma = pltpu.VMEM, pltpu.SemaphoreType.DMA
        local = (len_i, len_j, len_k)
        res = pl.pallas_call(
            functools.partial(kernel, n1, n2),
            out_shape=outs,
            in_specs=[any_spec] * 8,
            out_specs=[vmem_spec] * 4 + [any_spec] * (len(outs) - 4),
            scratch_shapes=[
                vmem((2, m1, m1), BF16), vmem((2, m2, m2), BF16), vmem((2, 2, len_k, len_k), BF16), vmem(local, F32),
                vmem((blk_j * blk_j, blk_j * blk_j), BF16),
                vmem((m1, blk_j, len_k), BF16), vmem((blk_i, m2, len_k), BF16),
                vmem((blk_j, m1, len_k), BF16), vmem((blk_j, m1, len_k), BF16),
                vmem((2, SLOTS, m1, blk_j, len_k), BF16), vmem((2, SLOTS, blk_i, m2, len_k), BF16),
                vmem(local, BF16), vmem(local, BF16), vmem(local, BF16), vmem(local, BF16),
                vmem(local, BF16),
                dma((2, rhs, n1 + n2 - 1)), dma((2, rhs, n1 + n2 - 1)),
                dma((2, rhs, n1 + n2 - 2)), dma((2, rhs, n1 + n2 - 2)),
                dma((2, SLOTS, 2)), dma((12,)),
            ],
            compiler_params=pltpu.CompilerParams(collective_id=0, has_side_effects=True, vmem_limit_bytes=46 * 1024 * 1024),
            name='kron',
        )(x_vol, diag_vals, a1, a2, a3, b1, b2, b3)
        return pl.pallas_call(
            finish,
            out_shape=jax.ShapeDtypeStruct(x_vol.shape, F32),
            in_specs=[vmem_spec] * 4,
            out_specs=any_spec,
            scratch_shapes=[vmem(local, F32), dma((rhs,))],
            compiler_params=pltpu.CompilerParams(vmem_limit_bytes=8 * 1024 * 1024),
            name='finish',
        )(*res[:4])

    return jax.shard_map(local_op, mesh=mesh, in_specs=(vol_spec, diag_spec, P(), P(), P(), P(), P(), P()), out_specs=vol_spec, check_vma=False)
```

```python
import functools

import jax
import jax.numpy as jnp
from jax import lax
from jax.experimental import pallas as pl
from jax.experimental.pallas import tpu as pltpu
from jax.sharding import PartitionSpec as P

BF16, F32 = jnp.bfloat16, jnp.float32
AHEAD = 2
SLOTS = 2
PER = 2


def kernel(n1, n2, x, d, a1, a2, a3, b1, b2, b3, z, third_last, ty_last, tx_last, w, ly, lx, lc, ty, tx,
           f1, f2, g, dv, perm, buf_y, buf_x, mid_a, mid_b, out_y, out_x, vb, cb, yb, xb, ws,
           in_send, in_recv, out_send, out_recv, own_sem, ld):
    rhs, len_i, len_j, len_k = x.shape
    blk_j, blk_i = len_j // n1, len_i // n2
    me_y, me_x, me_c = lax.axis_index('mode1'), lax.axis_index('mode2'), lax.axis_index('mode3')
    other = 1 - me_c
    chunks = rhs // PER
    order_y = [o for o in (1, n1 - 1, *range(2, n1 - 1))]
    order_x = [o for o in (1, n2 - 1, *range(2, n2 - 1))]

    def peer_y(o):
        return lax.rem(me_y + o, n1)

    def peer_x(o):
        return lax.rem(me_x + o, n2)

    def al(v, m):
        return pl.multiple_of(v * m, m)

    def remote(src, dst, send, recv, axis, index):
        return pltpu.make_async_remote_copy(src_ref=src, dst_ref=dst, send_sem=send, recv_sem=recv,
                                            device_id={axis: index}, device_id_type=pl.DeviceIdType.MESH)

    def in_copies(s, v, r):
        y_list, x_list = [], []
        group = pl.ds(r * PER, PER)
        for o in order_y:
            q = peer_y(o)
            y_list.append(remote(v.at[group, :, pl.ds(al(q, blk_j), blk_j), :], ly.at[s, group, pl.ds(al(me_y, len_i), len_i)],
                                 in_send.at[s, r, o - 1], in_recv.at[s, r, o - 1], 'mode1', q))
        for o in order_x:
            p = peer_x(o)
            x_list.append(remote(v.at[group, pl.ds(al(p, blk_i), blk_i)], lx.at[s, group, :, pl.ds(al(me_x, len_j), len_j), :],
                                 in_send.at[s, r, n1 + o - 2], in_recv.at[s, r, n1 + o - 2], 'mode2', p))
        core = remote(v.at[group], lc.at[s, group], in_send.at[s, r, n1 + n2 - 2], in_recv.at[s, r, n1 + n2 - 2], 'mode3', other)
        return y_list, x_list, core

    def send_in(s, v, r):
        y_list, x_list, core = in_copies(s, v, r)
        for pair in zip(x_list, y_list):
            for copy in pair:
                copy.start()
        core.start()

    def out_x_copies(s, r, slot, last=False):
        copies = []
        home = tx_last if last else tx.at[s, pl.ds(r * PER, PER)]
        for o in order_x:
            p = peer_x(o)
            copies.append(remote(out_x.at[s, slot, :, :, pl.ds(al(p, len_j), len_j), :], home.at[:, pl.ds(al(me_x, blk_i), blk_i)],
                                 out_send.at[s, r, n1 + o - 2], out_recv.at[s, r, n1 + o - 2], 'mode2', p))
        if last:
            return copies, None
        own = pltpu.make_async_copy(out_x.at[s, slot, :, :, pl.ds(al(me_x, len_j), len_j), :],
                                    home.at[:, pl.ds(al(me_x, blk_i), blk_i)], own_sem.at[s, slot, 1])
        return copies, own

    def out_y_copies(s, r, slot, last=False):
        copies = []
        home = ty_last if last else ty.at[s, pl.ds(r * PER, PER)]
        for o in order_y:
            q = peer_y(o)
            copies.append(remote(out_y.at[s, slot, :, pl.ds(al(q, len_i), len_i)], home.at[:, :, pl.ds(al(me_y, blk_j), blk_j), :],
                                 out_send.at[s, r, o - 1], out_recv.at[s, r, o - 1], 'mode1', q))
        if last:
            return copies, None
        own = pltpu.make_async_copy(out_y.at[s, slot, :, pl.ds(al(me_y, len_i), len_i)],
                                    home.at[:, :, pl.ds(al(me_y, blk_j), blk_j), :], own_sem.at[s, slot, 0])
        return copies, own

    def products(s, v, r, last=False):
        slot = lax.rem(r, SLOTS)
        y_list, x_list, _ = in_copies(s, v, r)
        for copy in x_list + y_list:
            copy.wait_send()
            copy.wait_recv()
        blocks = buf_y.shape[0] // blk_j

        def loads_of(t):
            first, second = [], []
            for o in range(n2):
                p = peer_x(o)
                src = v.at[t, pl.ds(al(me_x, blk_i), blk_i)] if o == 0 else lx.at[s, t, :, pl.ds(al(p, len_j), len_j), :]
                first.append(pltpu.make_async_copy(src, buf_x.at[:, pl.ds(al(p, len_j), len_j), :], ld.at[n1 + o]))
            for o in range(n1):
                q = peer_y(o)
                src = v.at[t, :, pl.ds(al(me_y, blk_j), blk_j), :] if o == 0 else ly.at[s, t, pl.ds(al(q, len_i), len_i)]
                second.append(pltpu.make_async_copy(src, buf_y.at[pl.ds(al(q, len_i), len_i)], ld.at[o]))
            return first, second

        @pl.loop(0, PER)
        def _(c):
            first, second = loads_of(r * PER + c)
            for copy in first + second:
                copy.start()
            for copy in first:
                copy.wait()

            @pl.loop(0, blk_i)
            def _(i):
                out_x[s, slot, c, i] = jnp.dot(f2[s], buf_x[i], preferred_element_type=F32).astype(BF16)

            for copy in second:
                copy.wait()

            @pl.loop(0, blocks)
            def _(b):
                rows = pl.ds(al(b, blk_j), blk_j)
                block = buf_y[rows].reshape(blk_j * blk_j, len_k)
                mid_a[:, rows, :] = jnp.dot(perm[...], block, preferred_element_type=F32).astype(BF16).reshape(blk_j, blk_j, len_k)

            @pl.loop(0, blk_j)
            def _(j):
                mid_b[j] = jnp.dot(f1[s], mid_a[j], preferred_element_type=F32).astype(BF16)

            @pl.loop(0, blocks)
            def _(b):
                rows = pl.ds(al(b, blk_j), blk_j)
                block = mid_b[:, rows, :].reshape(blk_j * blk_j, len_k)
                out_y[s, slot, c, rows] = jnp.dot(perm[...], block, preferred_element_type=F32).astype(BF16).reshape(blk_j, blk_j, len_k)

        copies_x, own_x = out_x_copies(s, r, slot, last)
        copies_y, own_y = out_y_copies(s, r, slot, last)
        for pair in zip(copies_x, copies_y):
            for copy in pair:
                copy.start()
        if last:
            tx_last[:, pl.ds(al(me_x, blk_i), blk_i)] = out_x[s, slot, :, :, pl.ds(al(me_x, len_j), len_j), :]
            ty_last[:, :, pl.ds(al(me_y, blk_j), blk_j), :] = out_y[s, slot, :, pl.ds(al(me_y, len_i), len_i)]
        else:
            own_x.start()
            own_y.start()

    step = max(1, 256 // len_j)
    flat = (step * len_j, len_k)

    def wait_core(s, v, r):
        core = in_copies(s, v, r)[2]
        core.wait_send()
        core.wait_recv()

    def wait_out(s, r, last=False):
        slot = lax.rem(r, SLOTS)
        copies_x, own_x = out_x_copies(s, r, slot, last)
        copies_y, own_y = out_y_copies(s, r, slot, last)
        for copy in copies_x + copies_y:
            copy.wait_send()
            copy.wait_recv()
        if not last:
            own_x.wait()
            own_y.wait()

    def mode3(s, rows):
        return (jnp.dot(vb[rows].reshape(flat), g[s, 0], preferred_element_type=F32)
                + jnp.dot(cb[rows].reshape(flat), g[s, 1], preferred_element_type=F32)).astype(BF16)

    def combine(s, v, r):
        wait_core(s, v, r)
        wait_out(s, r)

        @pl.loop(0, PER)
        def _(c):
            t = r * PER + c
            loads = [pltpu.make_async_copy(src, dst, ld.at[n]) for n, (src, dst) in enumerate(
                ((v.at[t], vb), (lc.at[s, t], cb), (ty.at[s, t], yb), (tx.at[s, t], xb)))]
            for copy in loads:
                copy.start()
            for copy in loads:
                copy.wait()

            @pl.loop(0, len_i // step)
            def _(b):
                rows = pl.ds(b * step, step)
                total = (yb[rows].reshape(flat).astype(F32) + xb[rows].reshape(flat).astype(F32)) + mode3(s, rows).astype(F32)
                if s == 0:
                    scaled = dv[rows].reshape(flat) * total.astype(BF16).astype(F32)
                    ws[rows] = scaled.astype(BF16).reshape(step, len_j, len_k)
                else:
                    z[t, rows] = total.reshape(step, len_j, len_k)

            if s == 0:
                store = pltpu.make_async_copy(ws, w.at[t], ld.at[0])
                store.start()
                store.wait()

    barrier = pltpu.get_barrier_semaphore()
    for o in range(1, n1):
        pl.semaphore_signal(barrier, inc=1, device_id={'mode1': peer_y(o)}, device_id_type=pl.DeviceIdType.MESH)
    for o in range(1, n2):
        pl.semaphore_signal(barrier, inc=1, device_id={'mode2': peer_x(o)}, device_id_type=pl.DeviceIdType.MESH)
    pl.semaphore_signal(barrier, inc=1, device_id={'mode3': other}, device_id_type=pl.DeviceIdType.MESH)
    pl.semaphore_wait(barrier, n1 + n2 - 1)

    for r in range(AHEAD):
        send_in(0, x, r)

    mine, theirs = pl.ds(al(me_c, len_k), len_k), pl.ds(al(other, len_k), len_k)
    loads = [pltpu.make_async_copy(src, dst, ld.at[n]) for n, (src, dst) in enumerate((
        (a1, f1.at[0]), (b1, f1.at[1]), (a2, f2.at[0]), (b2, f2.at[1]), (d, dv),
        (a3.at[mine, mine], g.at[0, 0]), (a3.at[mine, theirs], g.at[0, 1]),
        (b3.at[mine, mine], g.at[1, 0]), (b3.at[mine, theirs], g.at[1, 1])))]
    for copy in loads:
        copy.start()
    size = blk_j * blk_j
    row = lax.broadcasted_iota(jnp.int32, (size, size), 0)
    col = lax.broadcasted_iota(jnp.int32, (size, size), 1)
    perm[...] = jnp.where(col == lax.rem(row, blk_j) * blk_j + row // blk_j, 1.0, 0.0).astype(BF16)
    for copy in loads:
        copy.wait()
    for s in range(2):
        for c in range(2):
            g[s, c] = g[s, c].astype(F32).T.astype(BF16)

    @pl.loop(0, chunks + 1)
    def _(n):
        @pl.when(n < chunks)
        def _():
            products(0, x, n)

        @pl.when(n + AHEAD < chunks)
        def _():
            send_in(0, x, n + AHEAD)

        @pl.when(n >= 1)
        def _():
            combine(0, x, n - 1)
            send_in(1, w, n - 1)

        @pl.when(n >= 2)
        def _():
            products(1, w, n - 2)

        @pl.when(n >= 3)
        def _():
            combine(1, w, n - 3)

    last = chunks - 1
    products(1, w, last, True)
    combine(1, w, last - 1)
    wait_core(1, w, last)

    @pl.loop(0, PER)
    def _(c):
        t = last * PER + c
        loads = [pltpu.make_async_copy(w.at[t], vb, ld.at[0]), pltpu.make_async_copy(lc.at[1, t], cb, ld.at[1])]
        for copy in loads:
            copy.start()
        for copy in loads:
            copy.wait()

        @pl.loop(0, len_i // step)
        def _(b):
            rows = pl.ds(b * step, step)
            third_last[c, rows] = mode3(1, rows).reshape(step, len_j, len_k)

    wait_out(1, last, True)


def finish(z_first, third, ty, tx, z, zb, sem):
    done, len_i = z_first.shape[0], z_first.shape[1]
    writes = [pltpu.make_async_copy(z_first.at[r], z.at[r], sem.at[r]) for r in range(done)]
    for copy in writes:
        copy.start()
    for c in range(third.shape[0]):
        @pl.loop(0, len_i)
        def _(i):
            zb[c, i] = (ty[c, i].astype(F32) + tx[c, i].astype(F32)) + third[c, i].astype(F32)

        writes.append(pltpu.make_async_copy(zb.at[c], z.at[done + c], sem.at[done + c]))
        writes[-1].start()
    for copy in writes:
        copy.wait()


def solution(mesh):
    n1, n2, n3 = mesh.shape['mode1'], mesh.shape['mode2'], mesh.shape['mode3']
    vol_spec = P('rhs', 'mode1', 'mode2', 'mode3')
    diag_spec = P('mode1', 'mode2', 'mode3')

    def local_op(x_vol, diag_vals, a1, a2, a3, b1, b2, b3):
        rhs, len_i, len_j, len_k = x_vol.shape
        m1, m2 = len_i * n1, len_j * n2
        blk_j, blk_i = len_j // n1, len_i // n2
        any_spec = pl.BlockSpec(memory_space=pl.ANY)
        vmem_spec = pl.BlockSpec(memory_space=pltpu.VMEM)
        outs = [
            pltpu.VMEM((rhs - PER, len_i, len_j, len_k), F32),
            *[pltpu.VMEM((PER, len_i, len_j, len_k), BF16)] * 3,
            jax.ShapeDtypeStruct((rhs, len_i, len_j, len_k), BF16),
            jax.ShapeDtypeStruct((2, rhs, m1, blk_j, len_k), BF16),
            jax.ShapeDtypeStruct((2, rhs, blk_i, m2, len_k), BF16),
            jax.ShapeDtypeStruct((2, rhs, len_i, len_j, len_k), BF16),
            jax.ShapeDtypeStruct((2, rhs, len_i, len_j, len_k), BF16),
            jax.ShapeDtypeStruct((2, rhs, len_i, len_j, len_k), BF16),
        ]
        vmem, dma = pltpu.VMEM, pltpu.SemaphoreType.DMA
        local = (len_i, len_j, len_k)
        res = pl.pallas_call(
            functools.partial(kernel, n1, n2),
            out_shape=outs,
            in_specs=[any_spec] * 8,
            out_specs=[vmem_spec] * 4 + [any_spec] * (len(outs) - 4),
            scratch_shapes=[
                vmem((2, m1, m1), BF16), vmem((2, m2, m2), BF16), vmem((2, 2, len_k, len_k), BF16), vmem(local, F32),
                vmem((blk_j * blk_j, blk_j * blk_j), BF16),
                vmem((m1, blk_j, len_k), BF16), vmem((blk_i, m2, len_k), BF16),
                vmem((blk_j, m1, len_k), BF16), vmem((blk_j, m1, len_k), BF16),
                vmem((2, SLOTS, PER, m1, blk_j, len_k), BF16), vmem((2, SLOTS, PER, blk_i, m2, len_k), BF16),
                vmem(local, BF16), vmem(local, BF16), vmem(local, BF16), vmem(local, BF16),
                vmem(local, BF16),
                dma((2, rhs // PER, n1 + n2 - 1)), dma((2, rhs // PER, n1 + n2 - 1)),
                dma((2, rhs // PER, n1 + n2 - 2)), dma((2, rhs // PER, n1 + n2 - 2)),
                dma((2, SLOTS, 2)), dma((12,)),
            ],
            compiler_params=pltpu.CompilerParams(collective_id=0, has_side_effects=True, vmem_limit_bytes=45 * 1024 * 1024),
            name='kron',
        )(x_vol, diag_vals, a1, a2, a3, b1, b2, b3)
        return pl.pallas_call(
            finish,
            out_shape=jax.ShapeDtypeStruct(x_vol.shape, F32),
            in_specs=[vmem_spec] * 4,
            out_specs=any_spec,
            scratch_shapes=[vmem((PER, *local), F32), dma((rhs,))],
            compiler_params=pltpu.CompilerParams(vmem_limit_bytes=8 * 1024 * 1024),
            name='finish',
        )(*res[:4])

    return jax.shard_map(local_op, mesh=mesh, in_specs=(vol_spec, diag_spec, P(), P(), P(), P(), P(), P()), out_specs=vol_spec, check_vma=False)
```

```python
import functools

import jax
import jax.numpy as jnp
from jax import lax
from jax.experimental import pallas as pl
from jax.experimental.pallas import tpu as pltpu
from jax.sharding import PartitionSpec as P

BF16, F32 = jnp.bfloat16, jnp.float32
AHEAD = 2
SLOTS = 2
PER = 2


def kernel(n1, n2, x, d, a1, a2, a3, b1, b2, b3, z, third_last, ty_last, tx_last, w, ly, lx, lc, ty, tx,
           f1, f2, g, dv, perm, buf_y, buf_x, mid_a, mid_b, out_y, out_x, vb, cb, yb, xb, ws,
           in_send, in_recv, out_send, out_recv, own_sem, ld):
    rhs, len_i, len_j, len_k = x.shape
    blk_j, blk_i = len_j // n1, len_i // n2
    me_y, me_x, me_c = lax.axis_index('mode1'), lax.axis_index('mode2'), lax.axis_index('mode3')
    other = 1 - me_c
    chunks = rhs // PER

    def send_order(n):
        near_first, far_first = (1, n - 1, *range(2, n - 1)), (*range(2, n - 1), 1, n - 1)
        return [a + me_c * (b - a) for a, b in zip(near_first, far_first)]

    order_y, order_x = send_order(n1), send_order(n2)
    all_y, all_x = range(1, n1), range(1, n2)

    def peer_y(o):
        return lax.rem(me_y + o, n1)

    def peer_x(o):
        return lax.rem(me_x + o, n2)

    def al(v, m):
        return pl.multiple_of(v * m, m)

    def remote(src, dst, send, recv, axis, index):
        return pltpu.make_async_remote_copy(src_ref=src, dst_ref=dst, send_sem=send, recv_sem=recv,
                                            device_id={axis: index}, device_id_type=pl.DeviceIdType.MESH)

    def in_copies(s, v, r, offsets_y=all_y, offsets_x=all_x):
        y_list, x_list = [], []
        group = pl.ds(r * PER, PER)
        for o in offsets_y:
            q = peer_y(o)
            y_list.append(remote(v.at[group, :, pl.ds(al(q, blk_j), blk_j), :], ly.at[s, group, pl.ds(al(me_y, len_i), len_i)],
                                 in_send.at[s, r, o - 1], in_recv.at[s, r, o - 1], 'mode1', q))
        for o in offsets_x:
            p = peer_x(o)
            x_list.append(remote(v.at[group, pl.ds(al(p, blk_i), blk_i)], lx.at[s, group, :, pl.ds(al(me_x, len_j), len_j), :],
                                 in_send.at[s, r, n1 + o - 2], in_recv.at[s, r, n1 + o - 2], 'mode2', p))
        core = remote(v.at[group], lc.at[s, group], in_send.at[s, r, n1 + n2 - 2], in_recv.at[s, r, n1 + n2 - 2], 'mode3', other)
        return y_list, x_list, core

    def send_in(s, v, r):
        y_list, x_list, core = in_copies(s, v, r, order_y, order_x)
        for pair in zip(x_list, y_list):
            for copy in pair:
                copy.start()
        core.start()

    def out_x_copies(s, r, slot, last=False, offsets=all_x):
        copies = []
        home = tx_last if last else tx.at[s, pl.ds(r * PER, PER)]
        for o in offsets:
            p = peer_x(o)
            copies.append(remote(out_x.at[s, slot, :, :, pl.ds(al(p, len_j), len_j), :], home.at[:, pl.ds(al(me_x, blk_i), blk_i)],
                                 out_send.at[s, r, n1 + o - 2], out_recv.at[s, r, n1 + o - 2], 'mode2', p))
        if last:
            return copies, None
        own = pltpu.make_async_copy(out_x.at[s, slot, :, :, pl.ds(al(me_x, len_j), len_j), :],
                                    home.at[:, pl.ds(al(me_x, blk_i), blk_i)], own_sem.at[s, slot, 1])
        return copies, own

    def out_y_copies(s, r, slot, last=False, offsets=all_y):
        copies = []
        home = ty_last if last else ty.at[s, pl.ds(r * PER, PER)]
        for o in offsets:
            q = peer_y(o)
            copies.append(remote(out_y.at[s, slot, :, pl.ds(al(q, len_i), len_i)], home.at[:, :, pl.ds(al(me_y, blk_j), blk_j), :],
                                 out_send.at[s, r, o - 1], out_recv.at[s, r, o - 1], 'mode1', q))
        if last:
            return copies, None
        own = pltpu.make_async_copy(out_y.at[s, slot, :, pl.ds(al(me_y, len_i), len_i)],
                                    home.at[:, :, pl.ds(al(me_y, blk_j), blk_j), :], own_sem.at[s, slot, 0])
        return copies, own

    def products(s, v, r, last=False):
        slot = lax.rem(r, SLOTS)
        y_list, x_list, _ = in_copies(s, v, r)
        for copy in x_list + y_list:
            copy.wait_send()
            copy.wait_recv()
        blocks = buf_y.shape[0] // blk_j

        def loads_of(t):
            first, second = [], []
            for o in range(n2):
                p = peer_x(o)
                src = v.at[t, pl.ds(al(me_x, blk_i), blk_i)] if o == 0 else lx.at[s, t, :, pl.ds(al(p, len_j), len_j), :]
                first.append(pltpu.make_async_copy(src, buf_x.at[:, pl.ds(al(p, len_j), len_j), :], ld.at[n1 + o]))
            for o in range(n1):
                q = peer_y(o)
                src = v.at[t, :, pl.ds(al(me_y, blk_j), blk_j), :] if o == 0 else ly.at[s, t, pl.ds(al(q, len_i), len_i)]
                second.append(pltpu.make_async_copy(src, buf_y.at[pl.ds(al(q, len_i), len_i)], ld.at[o]))
            return first, second

        @pl.loop(0, PER)
        def _(c):
            first, second = loads_of(r * PER + c)
            for copy in first + second:
                copy.start()
            for copy in first:
                copy.wait()

            @pl.loop(0, blk_i)
            def _(i):
                out_x[s, slot, c, i] = jnp.dot(f2[s], buf_x[i], preferred_element_type=F32).astype(BF16)

            for copy in second:
                copy.wait()

            @pl.loop(0, blocks)
            def _(b):
                rows = pl.ds(al(b, blk_j), blk_j)
                block = buf_y[rows].reshape(blk_j * blk_j, len_k)
                mid_a[:, rows, :] = jnp.dot(perm[...], block, preferred_element_type=F32).astype(BF16).reshape(blk_j, blk_j, len_k)

            @pl.loop(0, blk_j)
            def _(j):
                mid_b[j] = jnp.dot(f1[s], mid_a[j], preferred_element_type=F32).astype(BF16)

            @pl.loop(0, blocks)
            def _(b):
                rows = pl.ds(al(b, blk_j), blk_j)
                block = mid_b[:, rows, :].reshape(blk_j * blk_j, len_k)
                out_y[s, slot, c, rows] = jnp.dot(perm[...], block, preferred_element_type=F32).astype(BF16).reshape(blk_j, blk_j, len_k)

        copies_x, own_x = out_x_copies(s, r, slot, last, order_x)
        copies_y, own_y = out_y_copies(s, r, slot, last, order_y)
        for pair in zip(copies_x, copies_y):
            for copy in pair:
                copy.start()
        if last:
            tx_last[:, pl.ds(al(me_x, blk_i), blk_i)] = out_x[s, slot, :, :, pl.ds(al(me_x, len_j), len_j), :]
            ty_last[:, :, pl.ds(al(me_y, blk_j), blk_j), :] = out_y[s, slot, :, pl.ds(al(me_y, len_i), len_i)]
        else:
            own_x.start()
            own_y.start()

    step = max(1, 256 // len_j)
    flat = (step * len_j, len_k)

    def wait_core(s, v, r):
        core = in_copies(s, v, r)[2]
        core.wait_send()
        core.wait_recv()

    def wait_out(s, r, last=False):
        slot = lax.rem(r, SLOTS)
        copies_x, own_x = out_x_copies(s, r, slot, last)
        copies_y, own_y = out_y_copies(s, r, slot, last)
        for copy in copies_x + copies_y:
            copy.wait_send()
            copy.wait_recv()
        if not last:
            own_x.wait()
            own_y.wait()

    def mode3(s, rows):
        return (jnp.dot(vb[rows].reshape(flat), g[s, 0], preferred_element_type=F32)
                + jnp.dot(cb[rows].reshape(flat), g[s, 1], preferred_element_type=F32)).astype(BF16)

    def combine(s, v, r):
        wait_core(s, v, r)
        wait_out(s, r)

        @pl.loop(0, PER)
        def _(c):
            t = r * PER + c
            loads = [pltpu.make_async_copy(src, dst, ld.at[n]) for n, (src, dst) in enumerate(
                ((v.at[t], vb), (lc.at[s, t], cb), (ty.at[s, t], yb), (tx.at[s, t], xb)))]
            for copy in loads:
                copy.start()
            for copy in loads:
                copy.wait()

            @pl.loop(0, len_i // step)
            def _(b):
                rows = pl.ds(b * step, step)
                total = (yb[rows].reshape(flat).astype(F32) + xb[rows].reshape(flat).astype(F32)) + mode3(s, rows).astype(F32)
                if s == 0:
                    scaled = dv[rows].reshape(flat) * total.astype(BF16).astype(F32)
                    ws[rows] = scaled.astype(BF16).reshape(step, len_j, len_k)
                else:
                    z[t, rows] = total.reshape(step, len_j, len_k)

            if s == 0:
                store = pltpu.make_async_copy(ws, w.at[t], ld.at[0])
                store.start()
                store.wait()

    barrier = pltpu.get_barrier_semaphore()
    for o in range(1, n1):
        pl.semaphore_signal(barrier, inc=1, device_id={'mode1': peer_y(o)}, device_id_type=pl.DeviceIdType.MESH)
    for o in range(1, n2):
        pl.semaphore_signal(barrier, inc=1, device_id={'mode2': peer_x(o)}, device_id_type=pl.DeviceIdType.MESH)
    pl.semaphore_signal(barrier, inc=1, device_id={'mode3': other}, device_id_type=pl.DeviceIdType.MESH)
    pl.semaphore_wait(barrier, n1 + n2 - 1)

    for r in range(AHEAD):
        send_in(0, x, r)

    mine, theirs = pl.ds(al(me_c, len_k), len_k), pl.ds(al(other, len_k), len_k)
    loads = [pltpu.make_async_copy(src, dst, ld.at[n]) for n, (src, dst) in enumerate((
        (a1, f1.at[0]), (b1, f1.at[1]), (a2, f2.at[0]), (b2, f2.at[1]), (d, dv),
        (a3.at[mine, mine], g.at[0, 0]), (a3.at[mine, theirs], g.at[0, 1]),
        (b3.at[mine, mine], g.at[1, 0]), (b3.at[mine, theirs], g.at[1, 1])))]
    for copy in loads:
        copy.start()
    size = blk_j * blk_j
    row = lax.broadcasted_iota(jnp.int32, (size, size), 0)
    col = lax.broadcasted_iota(jnp.int32, (size, size), 1)
    perm[...] = jnp.where(col == lax.rem(row, blk_j) * blk_j + row // blk_j, 1.0, 0.0).astype(BF16)
    for copy in loads:
        copy.wait()
    for s in range(2):
        for c in range(2):
            g[s, c] = g[s, c].astype(F32).T.astype(BF16)

    @pl.loop(0, chunks + 1)
    def _(n):
        @pl.when(n < chunks)
        def _():
            products(0, x, n)

        @pl.when(n + AHEAD < chunks)
        def _():
            send_in(0, x, n + AHEAD)

        @pl.when(n >= 1)
        def _():
            combine(0, x, n - 1)
            send_in(1, w, n - 1)

        @pl.when(n >= 2)
        def _():
            products(1, w, n - 2)

        @pl.when(n >= 3)
        def _():
            combine(1, w, n - 3)

    last = chunks - 1
    products(1, w, last, True)
    combine(1, w, last - 1)
    wait_core(1, w, last)

    @pl.loop(0, PER)
    def _(c):
        t = last * PER + c
        loads = [pltpu.make_async_copy(w.at[t], vb, ld.at[0]), pltpu.make_async_copy(lc.at[1, t], cb, ld.at[1])]
        for copy in loads:
            copy.start()
        for copy in loads:
            copy.wait()

        @pl.loop(0, len_i // step)
        def _(b):
            rows = pl.ds(b * step, step)
            third_last[c, rows] = mode3(1, rows).reshape(step, len_j, len_k)

    wait_out(1, last, True)


def finish(z_first, third, ty, tx, z, zb, sem):
    done, len_i = z_first.shape[0], z_first.shape[1]
    writes = [pltpu.make_async_copy(z_first.at[r], z.at[r], sem.at[r]) for r in range(done)]
    for copy in writes:
        copy.start()
    for c in range(third.shape[0]):
        @pl.loop(0, len_i)
        def _(i):
            zb[c, i] = (ty[c, i].astype(F32) + tx[c, i].astype(F32)) + third[c, i].astype(F32)

        writes.append(pltpu.make_async_copy(zb.at[c], z.at[done + c], sem.at[done + c]))
        writes[-1].start()
    for copy in writes:
        copy.wait()


def solution(mesh):
    n1, n2, n3 = mesh.shape['mode1'], mesh.shape['mode2'], mesh.shape['mode3']
    vol_spec = P('rhs', 'mode1', 'mode2', 'mode3')
    diag_spec = P('mode1', 'mode2', 'mode3')

    def local_op(x_vol, diag_vals, a1, a2, a3, b1, b2, b3):
        rhs, len_i, len_j, len_k = x_vol.shape
        m1, m2 = len_i * n1, len_j * n2
        blk_j, blk_i = len_j // n1, len_i // n2
        any_spec = pl.BlockSpec(memory_space=pl.ANY)
        vmem_spec = pl.BlockSpec(memory_space=pltpu.VMEM)
        outs = [
            pltpu.VMEM((rhs - PER, len_i, len_j, len_k), F32),
            *[pltpu.VMEM((PER, len_i, len_j, len_k), BF16)] * 3,
            jax.ShapeDtypeStruct((rhs, len_i, len_j, len_k), BF16),
            jax.ShapeDtypeStruct((2, rhs, m1, blk_j, len_k), BF16),
            jax.ShapeDtypeStruct((2, rhs, blk_i, m2, len_k), BF16),
            jax.ShapeDtypeStruct((2, rhs, len_i, len_j, len_k), BF16),
            jax.ShapeDtypeStruct((2, rhs, len_i, len_j, len_k), BF16),
            jax.ShapeDtypeStruct((2, rhs, len_i, len_j, len_k), BF16),
        ]
        vmem, dma = pltpu.VMEM, pltpu.SemaphoreType.DMA
        local = (len_i, len_j, len_k)
        res = pl.pallas_call(
            functools.partial(kernel, n1, n2),
            out_shape=outs,
            in_specs=[any_spec] * 8,
            out_specs=[vmem_spec] * 4 + [any_spec] * (len(outs) - 4),
            scratch_shapes=[
                vmem((2, m1, m1), BF16), vmem((2, m2, m2), BF16), vmem((2, 2, len_k, len_k), BF16), vmem(local, F32),
                vmem((blk_j * blk_j, blk_j * blk_j), BF16),
                vmem((m1, blk_j, len_k), BF16), vmem((blk_i, m2, len_k), BF16),
                vmem((blk_j, m1, len_k), BF16), vmem((blk_j, m1, len_k), BF16),
                vmem((2, SLOTS, PER, m1, blk_j, len_k), BF16), vmem((2, SLOTS, PER, blk_i, m2, len_k), BF16),
                vmem(local, BF16), vmem(local, BF16), vmem(local, BF16), vmem(local, BF16),
                vmem(local, BF16),
                dma((2, rhs // PER, n1 + n2 - 1)), dma((2, rhs // PER, n1 + n2 - 1)),
                dma((2, rhs // PER, n1 + n2 - 2)), dma((2, rhs // PER, n1 + n2 - 2)),
                dma((2, SLOTS, 2)), dma((12,)),
            ],
            compiler_params=pltpu.CompilerParams(collective_id=0, has_side_effects=True, vmem_limit_bytes=45 * 1024 * 1024),
            name='kron',
        )(x_vol, diag_vals, a1, a2, a3, b1, b2, b3)
        return pl.pallas_call(
            finish,
            out_shape=jax.ShapeDtypeStruct(x_vol.shape, F32),
            in_specs=[vmem_spec] * 4,
            out_specs=any_spec,
            scratch_shapes=[vmem((PER, *local), F32), dma((rhs,))],
            compiler_params=pltpu.CompilerParams(vmem_limit_bytes=8 * 1024 * 1024),
            name='finish',
        )(*res[:4])

    return jax.shard_map(local_op, mesh=mesh, in_specs=(vol_spec, diag_spec, P(), P(), P(), P(), P(), P()), out_specs=vol_spec, check_vma=False)
```

```python
import functools

import jax
import jax.numpy as jnp
from jax import lax
from jax.experimental import pallas as pl
from jax.experimental.pallas import tpu as pltpu
from jax.sharding import PartitionSpec as P

BF16, F32 = jnp.bfloat16, jnp.float32
AHEAD = 2
SLOTS = 2
PER = 4


def kernel(n1, n2, x, d, a1, a2, a3, b1, b2, b3, z, third_last, ty_last, tx_last, w, ly, lx, lc, ty, tx,
           f1, f2, g, dv, buf_y, buf_x, mid_a, mid_b, out_y, out_x, vb, cb, yb, xb, ws,
           in_send, in_recv, out_send, out_recv, own_sem, ld):
    rhs, len_i, len_j, len_k = x.shape
    blk_j, blk_i = len_j // n1, len_i // n2
    me_y, me_x, me_c = lax.axis_index('mode1'), lax.axis_index('mode2'), lax.axis_index('mode3')
    other = 1 - me_c
    chunks = rhs // PER
    banks = out_y.shape[0]

    def send_order(n):
        near_first, far_first = (1, n - 1, *range(2, n - 1)), (*range(2, n - 1), 1, n - 1)
        return [a + me_c * (b - a) for a, b in zip(near_first, far_first)]

    order_y, order_x = send_order(n1), send_order(n2)
    all_y, all_x = range(1, n1), range(1, n2)

    def peer_y(o):
        return lax.rem(me_y + o, n1)

    def peer_x(o):
        return lax.rem(me_x + o, n2)

    def al(v, m):
        return pl.multiple_of(v * m, m)

    def remote(src, dst, send, recv, axis, index):
        return pltpu.make_async_remote_copy(src_ref=src, dst_ref=dst, send_sem=send, recv_sem=recv,
                                            device_id={axis: index}, device_id_type=pl.DeviceIdType.MESH)

    def in_copies(s, v, r, offsets_y=all_y, offsets_x=all_x):
        y_list, x_list = [], []
        group = pl.ds(r * PER, PER)
        for o in offsets_y:
            q = peer_y(o)
            y_list.append(remote(v.at[group, :, pl.ds(al(q, blk_j), blk_j), :], ly.at[s, group, pl.ds(al(me_y, len_i), len_i)],
                                 in_send.at[s, r, o - 1], in_recv.at[s, r, o - 1], 'mode1', q))
        for o in offsets_x:
            p = peer_x(o)
            x_list.append(remote(v.at[group, pl.ds(al(p, blk_i), blk_i)], lx.at[s, group, :, pl.ds(al(me_x, len_j), len_j), :],
                                 in_send.at[s, r, n1 + o - 2], in_recv.at[s, r, n1 + o - 2], 'mode2', p))
        core = remote(v.at[group], lc.at[s, group], in_send.at[s, r, n1 + n2 - 2], in_recv.at[s, r, n1 + n2 - 2], 'mode3', other)
        return y_list, x_list, core

    def send_in(s, v, r):
        y_list, x_list, core = in_copies(s, v, r, order_y, order_x)
        for pair in zip(x_list, y_list):
            for copy in pair:
                copy.start()
        core.start()

    def out_x_copies(s, r, slot, last=False, offsets=all_x):
        copies = []
        home = tx_last if last else tx.at[s, pl.ds(r * PER, PER)]
        for o in offsets:
            p = peer_x(o)
            copies.append(remote(out_x.at[s % banks, slot, :, :, pl.ds(al(p, len_j), len_j), :], home.at[:, pl.ds(al(me_x, blk_i), blk_i)],
                                 out_send.at[s, r, n1 + o - 2], out_recv.at[s, r, n1 + o - 2], 'mode2', p))
        if last:
            return copies, None
        own = pltpu.make_async_copy(out_x.at[s % banks, slot, :, :, pl.ds(al(me_x, len_j), len_j), :],
                                    home.at[:, pl.ds(al(me_x, blk_i), blk_i)], own_sem.at[s, slot, 1])
        return copies, own

    def out_y_copies(s, r, slot, last=False, offsets=all_y):
        copies = []
        home = ty_last if last else ty.at[s, pl.ds(r * PER, PER)]
        for o in offsets:
            q = peer_y(o)
            copies.append(remote(out_y.at[s % banks, slot, :, pl.ds(al(q, len_i), len_i)], home.at[:, :, pl.ds(al(me_y, blk_j), blk_j), :],
                                 out_send.at[s, r, o - 1], out_recv.at[s, r, o - 1], 'mode1', q))
        if last:
            return copies, None
        own = pltpu.make_async_copy(out_y.at[s % banks, slot, :, pl.ds(al(me_y, len_i), len_i)],
                                    home.at[:, :, pl.ds(al(me_y, blk_j), blk_j), :], own_sem.at[s, slot, 0])
        return copies, own

    def products(s, v, r, last=False):
        slot = lax.rem(r, SLOTS)
        y_list, x_list, _ = in_copies(s, v, r)
        for copy in x_list + y_list:
            copy.wait_send()
            copy.wait_recv()
        blocks = buf_y.shape[0] // blk_j

        def loads_of(t):
            first, second = [], []
            for o in range(n2):
                p = peer_x(o)
                src = v.at[t, pl.ds(al(me_x, blk_i), blk_i)] if o == 0 else lx.at[s, t, :, pl.ds(al(p, len_j), len_j), :]
                first.append(pltpu.make_async_copy(src, buf_x.at[:, pl.ds(al(p, len_j), len_j), :], ld.at[n1 + o]))
            for o in range(n1):
                q = peer_y(o)
                src = v.at[t, :, pl.ds(al(me_y, blk_j), blk_j), :] if o == 0 else ly.at[s, t, pl.ds(al(q, len_i), len_i)]
                second.append(pltpu.make_async_copy(src, buf_y.at[pl.ds(al(q, len_i), len_i)], ld.at[o]))
            return first, second

        @pl.loop(0, PER)
        def _(c):
            first, second = loads_of(r * PER + c)
            for copy in first + second:
                copy.start()
            for copy in first:
                copy.wait()

            @pl.loop(0, blk_i)
            def _(i):
                out_x[s % banks, slot, c, i] = jnp.dot(f2[s], buf_x[i], preferred_element_type=F32).astype(BF16)

            for copy in second:
                copy.wait()

            @pl.loop(0, blocks)
            def _(b):
                rows = pl.ds(al(b, blk_j), blk_j)
                mid_a[:, rows, :] = jnp.swapaxes(buf_y[rows], 0, 1)

            @pl.loop(0, blk_j)
            def _(j):
                mid_b[j] = jnp.dot(f1[s], mid_a[j], preferred_element_type=F32).astype(BF16)

            @pl.loop(0, blocks)
            def _(b):
                rows = pl.ds(al(b, blk_j), blk_j)
                out_y[s % banks, slot, c, rows] = jnp.swapaxes(mid_b[:, rows, :], 0, 1)

        copies_x, own_x = out_x_copies(s, r, slot, last, order_x)
        copies_y, own_y = out_y_copies(s, r, slot, last, order_y)
        for pair in zip(copies_x, copies_y):
            for copy in pair:
                copy.start()
        if last:
            tx_last[:, pl.ds(al(me_x, blk_i), blk_i)] = out_x[s % banks, slot, :, :, pl.ds(al(me_x, len_j), len_j), :]
            ty_last[:, :, pl.ds(al(me_y, blk_j), blk_j), :] = out_y[s % banks, slot, :, pl.ds(al(me_y, len_i), len_i)]
        else:
            own_x.start()
            own_y.start()

    step = max(1, 256 // len_j)
    flat = (step * len_j, len_k)

    def wait_core(s, v, r):
        core = in_copies(s, v, r)[2]
        core.wait_send()
        core.wait_recv()

    def wait_out(s, r, last=False):
        slot = lax.rem(r, SLOTS)
        copies_x, own_x = out_x_copies(s, r, slot, last)
        copies_y, own_y = out_y_copies(s, r, slot, last)
        for copy in copies_x + copies_y:
            copy.wait_send()
            copy.wait_recv()
        if not last:
            own_x.wait()
            own_y.wait()

    def mode3(s, rows):
        return (jnp.dot(vb[rows].reshape(flat), g[s, 0], preferred_element_type=F32)
                + jnp.dot(cb[rows].reshape(flat), g[s, 1], preferred_element_type=F32)).astype(BF16)

    def combine(s, v, r):
        wait_core(s, v, r)
        wait_out(s, r)

        @pl.loop(0, PER)
        def _(c):
            t = r * PER + c
            loads = [pltpu.make_async_copy(src, dst, ld.at[n]) for n, (src, dst) in enumerate(
                ((v.at[t], vb), (lc.at[s, t], cb), (ty.at[s, t], yb), (tx.at[s, t], xb)))]
            for copy in loads:
                copy.start()
            for copy in loads:
                copy.wait()

            @pl.loop(0, len_i // step)
            def _(b):
                rows = pl.ds(b * step, step)
                total = (yb[rows].reshape(flat).astype(F32) + xb[rows].reshape(flat).astype(F32)) + mode3(s, rows).astype(F32)
                if s == 0:
                    scaled = dv[rows].reshape(flat) * total.astype(BF16).astype(F32)
                    ws[rows] = scaled.astype(BF16).reshape(step, len_j, len_k)
                else:
                    z[t, rows] = total.reshape(step, len_j, len_k)

            if s == 0:
                store = pltpu.make_async_copy(ws, w.at[t], ld.at[0])
                store.start()
                store.wait()

    barrier = pltpu.get_barrier_semaphore()
    for o in range(1, n1):
        pl.semaphore_signal(barrier, inc=1, device_id={'mode1': peer_y(o)}, device_id_type=pl.DeviceIdType.MESH)
    for o in range(1, n2):
        pl.semaphore_signal(barrier, inc=1, device_id={'mode2': peer_x(o)}, device_id_type=pl.DeviceIdType.MESH)
    pl.semaphore_signal(barrier, inc=1, device_id={'mode3': other}, device_id_type=pl.DeviceIdType.MESH)
    pl.semaphore_wait(barrier, n1 + n2 - 1)

    for r in range(AHEAD):
        send_in(0, x, r)

    mine, theirs = pl.ds(al(me_c, len_k), len_k), pl.ds(al(other, len_k), len_k)
    loads = [pltpu.make_async_copy(src, dst, ld.at[n]) for n, (src, dst) in enumerate((
        (a1, f1.at[0]), (b1, f1.at[1]), (a2, f2.at[0]), (b2, f2.at[1]), (d, dv),
        (a3.at[mine, mine], g.at[0, 0]), (a3.at[mine, theirs], g.at[0, 1]),
        (b3.at[mine, mine], g.at[1, 0]), (b3.at[mine, theirs], g.at[1, 1])))]
    for copy in loads:
        copy.start()
    for copy in loads:
        copy.wait()
    for s in range(2):
        for c in range(2):
            g[s, c] = g[s, c].astype(F32).T.astype(BF16)

    @pl.loop(0, chunks + 1)
    def _(n):
        @pl.when(n < chunks)
        def _():
            products(0, x, n)

        @pl.when(n + AHEAD < chunks)
        def _():
            send_in(0, x, n + AHEAD)

        @pl.when(n >= 1)
        def _():
            combine(0, x, n - 1)
            send_in(1, w, n - 1)

        @pl.when(n >= 2)
        def _():
            products(1, w, n - 2)

        @pl.when(n >= 3)
        def _():
            combine(1, w, n - 3)

    last = chunks - 1
    products(1, w, last, True)
    combine(1, w, last - 1)
    wait_core(1, w, last)

    @pl.loop(0, PER)
    def _(c):
        t = last * PER + c
        loads = [pltpu.make_async_copy(w.at[t], vb, ld.at[0]), pltpu.make_async_copy(lc.at[1, t], cb, ld.at[1])]
        for copy in loads:
            copy.start()
        for copy in loads:
            copy.wait()

        @pl.loop(0, len_i // step)
        def _(b):
            rows = pl.ds(b * step, step)
            third_last[c, rows] = mode3(1, rows).reshape(step, len_j, len_k)

    wait_out(1, last, True)


def finish(z_first, third, ty, tx, z, zb, sem):
    done, len_i = z_first.shape[0], z_first.shape[1]
    writes = [pltpu.make_async_copy(z_first.at[r], z.at[r], sem.at[r]) for r in range(done)]
    for copy in writes:
        copy.start()
    for c in range(third.shape[0]):
        @pl.loop(0, len_i)
        def _(i):
            zb[c, i] = (ty[c, i].astype(F32) + tx[c, i].astype(F32)) + third[c, i].astype(F32)

        writes.append(pltpu.make_async_copy(zb.at[c], z.at[done + c], sem.at[done + c]))
        writes[-1].start()
    for copy in writes:
        copy.wait()


def solution(mesh):
    n1, n2, n3 = mesh.shape['mode1'], mesh.shape['mode2'], mesh.shape['mode3']
    vol_spec = P('rhs', 'mode1', 'mode2', 'mode3')
    diag_spec = P('mode1', 'mode2', 'mode3')

    def local_op(x_vol, diag_vals, a1, a2, a3, b1, b2, b3):
        rhs, len_i, len_j, len_k = x_vol.shape
        m1, m2 = len_i * n1, len_j * n2
        blk_j, blk_i = len_j // n1, len_i // n2
        banks = 1 if rhs // PER <= SLOTS else 2
        any_spec = pl.BlockSpec(memory_space=pl.ANY)
        vmem_spec = pl.BlockSpec(memory_space=pltpu.VMEM)
        outs = [
            pltpu.VMEM((rhs - PER, len_i, len_j, len_k), F32),
            *[pltpu.VMEM((PER, len_i, len_j, len_k), BF16)] * 3,
            jax.ShapeDtypeStruct((rhs, len_i, len_j, len_k), BF16),
            jax.ShapeDtypeStruct((2, rhs, m1, blk_j, len_k), BF16),
            jax.ShapeDtypeStruct((2, rhs, blk_i, m2, len_k), BF16),
            jax.ShapeDtypeStruct((2, rhs, len_i, len_j, len_k), BF16),
            jax.ShapeDtypeStruct((2, rhs, len_i, len_j, len_k), BF16),
            jax.ShapeDtypeStruct((2, rhs, len_i, len_j, len_k), BF16),
        ]
        vmem, dma = pltpu.VMEM, pltpu.SemaphoreType.DMA
        local = (len_i, len_j, len_k)
        res = pl.pallas_call(
            functools.partial(kernel, n1, n2),
            out_shape=outs,
            in_specs=[any_spec] * 8,
            out_specs=[vmem_spec] * 4 + [any_spec] * (len(outs) - 4),
            scratch_shapes=[
                vmem((2, m1, m1), BF16), vmem((2, m2, m2), BF16), vmem((2, 2, len_k, len_k), BF16), vmem(local, F32),
                vmem((m1, blk_j, len_k), BF16), vmem((blk_i, m2, len_k), BF16),
                vmem((blk_j, m1, len_k), BF16), vmem((blk_j, m1, len_k), BF16),
                vmem((banks, SLOTS, PER, m1, blk_j, len_k), BF16), vmem((banks, SLOTS, PER, blk_i, m2, len_k), BF16),
                vmem(local, BF16), vmem(local, BF16), vmem(local, BF16), vmem(local, BF16),
                vmem(local, BF16),
                dma((2, rhs // PER, n1 + n2 - 1)), dma((2, rhs // PER, n1 + n2 - 1)),
                dma((2, rhs // PER, n1 + n2 - 2)), dma((2, rhs // PER, n1 + n2 - 2)),
                dma((2, SLOTS, 2)), dma((12,)),
            ],
            compiler_params=pltpu.CompilerParams(collective_id=0, has_side_effects=True, vmem_limit_bytes=42 * 1024 * 1024),
            name='kron',
        )(x_vol, diag_vals, a1, a2, a3, b1, b2, b3)
        return pl.pallas_call(
            finish,
            out_shape=jax.ShapeDtypeStruct(x_vol.shape, F32),
            in_specs=[vmem_spec] * 4,
            out_specs=any_spec,
            scratch_shapes=[vmem((PER, *local), F32), dma((rhs,))],
            compiler_params=pltpu.CompilerParams(vmem_limit_bytes=12 * 1024 * 1024),
            name='finish',
        )(*res[:4])

    return jax.shard_map(local_op, mesh=mesh, in_specs=(vol_spec, diag_spec, P(), P(), P(), P(), P(), P()), out_specs=vol_spec, check_vma=False)
```

```python
import functools

import jax
import jax.numpy as jnp
from jax import lax
from jax.experimental import pallas as pl
from jax.experimental.pallas import tpu as pltpu
from jax.sharding import PartitionSpec as P

BF16, F32 = jnp.bfloat16, jnp.float32
AHEAD = 2
SLOTS = 2
PER = 4


def kernel(n1, n2, x, d, a1, a2, a3, b1, b2, b3, z, third_last, ty_last, tx_last, w, ly, lx, lc, ty, tx,
           f1, f2, g, dv, buf_y, buf_x, mid_a, mid_b, out_y, out_x, vb, cb, yb, xb, ws,
           in_send, in_recv, out_send, out_recv, own_sem, ld, w_sem):
    rhs, len_i, len_j, len_k = x.shape
    blk_j, blk_i = len_j // n1, len_i // n2
    me_y, me_x, me_c = lax.axis_index('mode1'), lax.axis_index('mode2'), lax.axis_index('mode3')
    other = 1 - me_c
    chunks = rhs // PER
    banks = out_y.shape[0]

    def send_order(n):
        near_first, far_first = (1, n - 1, *range(2, n - 1)), (*range(2, n - 1), 1, n - 1)
        return [a + me_c * (b - a) for a, b in zip(near_first, far_first)]

    order_y, order_x = send_order(n1), send_order(n2)
    all_y, all_x = range(1, n1), range(1, n2)

    def peer_y(o):
        return lax.rem(me_y + o, n1)

    def peer_x(o):
        return lax.rem(me_x + o, n2)

    def al(v, m):
        return pl.multiple_of(v * m, m)

    def remote(src, dst, send, recv, axis, index):
        return pltpu.make_async_remote_copy(src_ref=src, dst_ref=dst, send_sem=send, recv_sem=recv,
                                            device_id={axis: index}, device_id_type=pl.DeviceIdType.MESH)

    def in_copies(s, v, r, offsets_y=all_y, offsets_x=all_x):
        y_list, x_list = [], []
        group = pl.ds(r * PER, PER)
        for o in offsets_y:
            q = peer_y(o)
            y_list.append(remote(v.at[group, :, pl.ds(al(q, blk_j), blk_j), :], ly.at[s, group, pl.ds(al(me_y, len_i), len_i)],
                                 in_send.at[s, r, o - 1], in_recv.at[s, r, o - 1], 'mode1', q))
        for o in offsets_x:
            p = peer_x(o)
            x_list.append(remote(v.at[group, pl.ds(al(p, blk_i), blk_i)], lx.at[s, group, :, pl.ds(al(me_x, len_j), len_j), :],
                                 in_send.at[s, r, n1 + o - 2], in_recv.at[s, r, n1 + o - 2], 'mode2', p))
        core = remote(v.at[group], lc.at[s, group], in_send.at[s, r, n1 + n2 - 2], in_recv.at[s, r, n1 + n2 - 2], 'mode3', other)
        return y_list, x_list, core

    def send_in(s, v, r):
        y_list, x_list, core = in_copies(s, v, r, order_y, order_x)
        for pair in zip(x_list, y_list):
            for copy in pair:
                copy.start()
        core.start()

    def out_x_copies(s, r, slot, last=False, offsets=all_x):
        copies = []
        home = tx_last if last else tx.at[s, pl.ds(r * PER, PER)]
        for o in offsets:
            p = peer_x(o)
            copies.append(remote(out_x.at[s % banks, slot, :, :, pl.ds(al(p, len_j), len_j), :], home.at[:, pl.ds(al(me_x, blk_i), blk_i)],
                                 out_send.at[s, r, n1 + o - 2], out_recv.at[s, r, n1 + o - 2], 'mode2', p))
        if last:
            return copies, None
        own = pltpu.make_async_copy(out_x.at[s % banks, slot, :, :, pl.ds(al(me_x, len_j), len_j), :],
                                    home.at[:, pl.ds(al(me_x, blk_i), blk_i)], own_sem.at[s, slot, 1])
        return copies, own

    def out_y_copies(s, r, slot, last=False, offsets=all_y):
        copies = []
        home = ty_last if last else ty.at[s, pl.ds(r * PER, PER)]
        for o in offsets:
            q = peer_y(o)
            copies.append(remote(out_y.at[s % banks, slot, :, pl.ds(al(q, len_i), len_i)], home.at[:, :, pl.ds(al(me_y, blk_j), blk_j), :],
                                 out_send.at[s, r, o - 1], out_recv.at[s, r, o - 1], 'mode1', q))
        if last:
            return copies, None
        own = pltpu.make_async_copy(out_y.at[s % banks, slot, :, pl.ds(al(me_y, len_i), len_i)],
                                    home.at[:, :, pl.ds(al(me_y, blk_j), blk_j), :], own_sem.at[s, slot, 0])
        return copies, own

    def products(s, v, r, last=False):
        slot = lax.rem(r, SLOTS)
        y_list, x_list, _ = in_copies(s, v, r)
        for copy in x_list + y_list:
            copy.wait_send()
            copy.wait_recv()
        blocks = buf_y.shape[1] // blk_j

        def loads_of(c):
            t, half = r * PER + c, lax.rem(c, 2)
            first, second = [], []
            for o in range(n2):
                p = peer_x(o)
                src = v.at[t, pl.ds(al(me_x, blk_i), blk_i)] if o == 0 else lx.at[s, t, :, pl.ds(al(p, len_j), len_j), :]
                first.append(pltpu.make_async_copy(src, buf_x.at[half, :, pl.ds(al(p, len_j), len_j), :], ld.at[half, n1 + o]))
            for o in range(n1):
                q = peer_y(o)
                src = v.at[t, :, pl.ds(al(me_y, blk_j), blk_j), :] if o == 0 else ly.at[s, t, pl.ds(al(q, len_i), len_i)]
                second.append(pltpu.make_async_copy(src, buf_y.at[half, pl.ds(al(q, len_i), len_i)], ld.at[half, o]))
            return first, second

        def start_loads(c):
            first, second = loads_of(c)
            for copy in first + second:
                copy.start()

        start_loads(0)

        @pl.loop(0, PER)
        def _(c):
            half = lax.rem(c, 2)

            @pl.when(c + 1 < PER)
            def _():
                start_loads(c + 1)

            first, second = loads_of(c)
            for copy in first:
                copy.wait()

            @pl.loop(0, blk_i)
            def _(i):
                out_x[s % banks, slot, c, i] = jnp.dot(f2[s], buf_x[half, i], preferred_element_type=F32).astype(BF16)

            for copy in second:
                copy.wait()

            @pl.loop(0, blocks)
            def _(b):
                rows = pl.ds(al(b, blk_j), blk_j)
                mid_a[:, rows, :] = jnp.swapaxes(buf_y[half, rows], 0, 1)

            @pl.loop(0, blk_j)
            def _(j):
                mid_b[j] = jnp.dot(f1[s], mid_a[j], preferred_element_type=F32).astype(BF16)

            @pl.loop(0, blocks)
            def _(b):
                rows = pl.ds(al(b, blk_j), blk_j)
                out_y[s % banks, slot, c, rows] = jnp.swapaxes(mid_b[:, rows, :], 0, 1)

        copies_x, own_x = out_x_copies(s, r, slot, last, order_x)
        copies_y, own_y = out_y_copies(s, r, slot, last, order_y)
        for pair in zip(copies_x, copies_y):
            for copy in pair:
                copy.start()
        if last:
            tx_last[:, pl.ds(al(me_x, blk_i), blk_i)] = out_x[s % banks, slot, :, :, pl.ds(al(me_x, len_j), len_j), :]
            ty_last[:, :, pl.ds(al(me_y, blk_j), blk_j), :] = out_y[s % banks, slot, :, pl.ds(al(me_y, len_i), len_i)]
        else:
            own_x.start()
            own_y.start()

    step = max(1, 256 // len_j)
    flat = (step * len_j, len_k)

    def wait_core(s, v, r):
        core = in_copies(s, v, r)[2]
        core.wait_send()
        core.wait_recv()

    def wait_out(s, r, last=False):
        slot = lax.rem(r, SLOTS)
        copies_x, own_x = out_x_copies(s, r, slot, last)
        copies_y, own_y = out_y_copies(s, r, slot, last)
        for copy in copies_x + copies_y:
            copy.wait_send()
            copy.wait_recv()
        if not last:
            own_x.wait()
            own_y.wait()

    def mode3(s, half, rows):
        return (jnp.dot(vb[half, rows].reshape(flat), g[s, 0], preferred_element_type=F32)
                + jnp.dot(cb[half, rows].reshape(flat), g[s, 1], preferred_element_type=F32)).astype(BF16)

    def store_w(t):
        return pltpu.make_async_copy(ws, w.at[t], w_sem)

    def combine(s, v, r):
        wait_core(s, v, r)
        wait_out(s, r)

        def loads_of(c):
            t, half = r * PER + c, lax.rem(c, 2)
            return [pltpu.make_async_copy(src, dst.at[half], ld.at[half, n]) for n, (src, dst) in enumerate(
                ((v.at[t], vb), (lc.at[s, t], cb), (ty.at[s, t], yb), (tx.at[s, t], xb)))]

        for copy in loads_of(0):
            copy.start()

        @pl.loop(0, PER)
        def _(c):
            t, half = r * PER + c, lax.rem(c, 2)

            @pl.when(c + 1 < PER)
            def _():
                for copy in loads_of(c + 1):
                    copy.start()

            for copy in loads_of(c):
                copy.wait()
            if s == 0:
                @pl.when(c > 0)
                def _():
                    store_w(t - 1).wait()

            @pl.loop(0, len_i // step)
            def _(b):
                rows = pl.ds(b * step, step)
                total = (yb[half, rows].reshape(flat).astype(F32) + xb[half, rows].reshape(flat).astype(F32)) + mode3(s, half, rows).astype(F32)
                if s == 0:
                    scaled = dv[rows].reshape(flat) * total.astype(BF16).astype(F32)
                    ws[rows] = scaled.astype(BF16).reshape(step, len_j, len_k)
                else:
                    z[t, rows] = total.reshape(step, len_j, len_k)

            if s == 0:
                store_w(t).start()

        if s == 0:
            store_w(r * PER + PER - 1).wait()

    barrier = pltpu.get_barrier_semaphore()
    for o in range(1, n1):
        pl.semaphore_signal(barrier, inc=1, device_id={'mode1': peer_y(o)}, device_id_type=pl.DeviceIdType.MESH)
    for o in range(1, n2):
        pl.semaphore_signal(barrier, inc=1, device_id={'mode2': peer_x(o)}, device_id_type=pl.DeviceIdType.MESH)
    pl.semaphore_signal(barrier, inc=1, device_id={'mode3': other}, device_id_type=pl.DeviceIdType.MESH)
    pl.semaphore_wait(barrier, n1 + n2 - 1)

    for r in range(AHEAD):
        send_in(0, x, r)

    mine, theirs = pl.ds(al(me_c, len_k), len_k), pl.ds(al(other, len_k), len_k)
    loads = [pltpu.make_async_copy(src, dst, ld.at[0, n]) for n, (src, dst) in enumerate((
        (a1, f1.at[0]), (b1, f1.at[1]), (a2, f2.at[0]), (b2, f2.at[1]), (d, dv),
        (a3.at[mine, mine], g.at[0, 0]), (a3.at[mine, theirs], g.at[0, 1]),
        (b3.at[mine, mine], g.at[1, 0]), (b3.at[mine, theirs], g.at[1, 1])))]
    for copy in loads:
        copy.start()
    for copy in loads:
        copy.wait()
    for s in range(2):
        for c in range(2):
            g[s, c] = g[s, c].astype(F32).T.astype(BF16)

    @pl.loop(0, chunks + 1)
    def _(n):
        @pl.when(n < chunks)
        def _():
            products(0, x, n)

        @pl.when(n + AHEAD < chunks)
        def _():
            send_in(0, x, n + AHEAD)

        @pl.when(n >= 1)
        def _():
            combine(0, x, n - 1)
            send_in(1, w, n - 1)

        @pl.when(n >= 2)
        def _():
            products(1, w, n - 2)

        @pl.when(n >= 3)
        def _():
            combine(1, w, n - 3)

    last = chunks - 1
    products(1, w, last, True)
    combine(1, w, last - 1)
    wait_core(1, w, last)

    def last_loads(c):
        t, half = last * PER + c, lax.rem(c, 2)
        return [pltpu.make_async_copy(w.at[t], vb.at[half], ld.at[half, 0]), pltpu.make_async_copy(lc.at[1, t], cb.at[half], ld.at[half, 1])]

    for copy in last_loads(0):
        copy.start()

    @pl.loop(0, PER)
    def _(c):
        half = lax.rem(c, 2)

        @pl.when(c + 1 < PER)
        def _():
            for copy in last_loads(c + 1):
                copy.start()

        for copy in last_loads(c):
            copy.wait()

        @pl.loop(0, len_i // step)
        def _(b):
            rows = pl.ds(b * step, step)
            third_last[c, rows] = mode3(1, half, rows).reshape(step, len_j, len_k)

    wait_out(1, last, True)


def finish(z_first, third, ty, tx, z, zb, sem):
    done, len_i = z_first.shape[0], z_first.shape[1]
    writes = [pltpu.make_async_copy(z_first.at[r], z.at[r], sem.at[r]) for r in range(done)]
    for copy in writes:
        copy.start()
    for c in range(third.shape[0]):
        @pl.loop(0, len_i)
        def _(i):
            zb[c, i] = (ty[c, i].astype(F32) + tx[c, i].astype(F32)) + third[c, i].astype(F32)

        writes.append(pltpu.make_async_copy(zb.at[c], z.at[done + c], sem.at[done + c]))
        writes[-1].start()
    for copy in writes:
        copy.wait()


def solution(mesh):
    n1, n2, n3 = mesh.shape['mode1'], mesh.shape['mode2'], mesh.shape['mode3']
    vol_spec = P('rhs', 'mode1', 'mode2', 'mode3')
    diag_spec = P('mode1', 'mode2', 'mode3')

    def local_op(x_vol, diag_vals, a1, a2, a3, b1, b2, b3):
        rhs, len_i, len_j, len_k = x_vol.shape
        m1, m2 = len_i * n1, len_j * n2
        blk_j, blk_i = len_j // n1, len_i // n2
        banks = 1 if rhs // PER <= SLOTS else 2
        any_spec = pl.BlockSpec(memory_space=pl.ANY)
        vmem_spec = pl.BlockSpec(memory_space=pltpu.VMEM)
        outs = [
            pltpu.VMEM((rhs - PER, len_i, len_j, len_k), F32),
            *[pltpu.VMEM((PER, len_i, len_j, len_k), BF16)] * 3,
            jax.ShapeDtypeStruct((rhs, len_i, len_j, len_k), BF16),
            jax.ShapeDtypeStruct((2, rhs, m1, blk_j, len_k), BF16),
            jax.ShapeDtypeStruct((2, rhs, blk_i, m2, len_k), BF16),
            jax.ShapeDtypeStruct((2, rhs, len_i, len_j, len_k), BF16),
            jax.ShapeDtypeStruct((2, rhs, len_i, len_j, len_k), BF16),
            jax.ShapeDtypeStruct((2, rhs, len_i, len_j, len_k), BF16),
        ]
        vmem, dma = pltpu.VMEM, pltpu.SemaphoreType.DMA
        local = (len_i, len_j, len_k)
        res = pl.pallas_call(
            functools.partial(kernel, n1, n2),
            out_shape=outs,
            in_specs=[any_spec] * 8,
            out_specs=[vmem_spec] * 4 + [any_spec] * (len(outs) - 4),
            scratch_shapes=[
                vmem((2, m1, m1), BF16), vmem((2, m2, m2), BF16), vmem((2, 2, len_k, len_k), BF16), vmem(local, F32),
                vmem((2, m1, blk_j, len_k), BF16), vmem((2, blk_i, m2, len_k), BF16),
                vmem((blk_j, m1, len_k), BF16), vmem((blk_j, m1, len_k), BF16),
                vmem((banks, SLOTS, PER, m1, blk_j, len_k), BF16), vmem((banks, SLOTS, PER, blk_i, m2, len_k), BF16),
                *[vmem((2, *local), BF16)] * 4,
                vmem(local, BF16),
                dma((2, rhs // PER, n1 + n2 - 1)), dma((2, rhs // PER, n1 + n2 - 1)),
                dma((2, rhs // PER, n1 + n2 - 2)), dma((2, rhs // PER, n1 + n2 - 2)),
                dma((2, SLOTS, 2)), dma((2, 12)), dma,
            ],
            compiler_params=pltpu.CompilerParams(collective_id=0, has_side_effects=True, vmem_limit_bytes=42 * 1024 * 1024),
            name='kron',
        )(x_vol, diag_vals, a1, a2, a3, b1, b2, b3)
        return pl.pallas_call(
            finish,
            out_shape=jax.ShapeDtypeStruct(x_vol.shape, F32),
            in_specs=[vmem_spec] * 4,
            out_specs=any_spec,
            scratch_shapes=[vmem((PER, *local), F32), dma((rhs,))],
            compiler_params=pltpu.CompilerParams(vmem_limit_bytes=12 * 1024 * 1024),
            name='finish',
        )(*res[:4])

    return jax.shard_map(local_op, mesh=mesh, in_specs=(vol_spec, diag_spec, P(), P(), P(), P(), P(), P()), out_specs=vol_spec, check_vma=False)
```

```python
import functools

import jax
import jax.numpy as jnp
from jax import lax
from jax.experimental import pallas as pl
from jax.experimental.pallas import tpu as pltpu
from jax.sharding import PartitionSpec as P

BF16, F32 = jnp.bfloat16, jnp.float32
AHEAD = 2
SLOTS = 2
PER = 4


def kernel(n1, n2, x, d, a1, a2, a3, b1, b2, b3, z, third_last, ty_last, tx_last, w, ly, lx, lc, ty, tx,
           f1, f2, g, dv, buf_y, buf_x, mid_a, mid_b, out_y, out_x, vb, cb, yb, xb, ws,
           in_send, in_recv, out_send, out_recv, own_sem, ld, w_sem):
    rhs, len_i, len_j, len_k = x.shape
    blk_j, blk_i = len_j // n1, len_i // n2
    me_y, me_x, me_c = lax.axis_index('mode1'), lax.axis_index('mode2'), lax.axis_index('mode3')
    other = 1 - me_c
    chunks = rhs // PER
    banks = out_y.shape[0]

    def send_order(n):
        near_first, far_first = (1, n - 1, *range(2, n - 1)), (*range(2, n - 1), 1, n - 1)
        return [a + me_c * (b - a) for a, b in zip(near_first, far_first)]

    order_y, order_x = send_order(n1), send_order(n2)
    all_y, all_x = range(1, n1), range(1, n2)

    def peer_y(o):
        return lax.rem(me_y + o, n1)

    def peer_x(o):
        return lax.rem(me_x + o, n2)

    def al(v, m):
        return pl.multiple_of(v * m, m)

    def remote(src, dst, send, recv, axis, index):
        return pltpu.make_async_remote_copy(src_ref=src, dst_ref=dst, send_sem=send, recv_sem=recv,
                                            device_id={axis: index}, device_id_type=pl.DeviceIdType.MESH)

    def in_copies(s, v, r, offsets_y=all_y, offsets_x=all_x):
        y_list, x_list = [], []
        group = pl.ds(r * PER, PER)
        for o in offsets_y:
            q = peer_y(o)
            y_list.append(remote(v.at[group, :, pl.ds(al(q, blk_j), blk_j), :], ly.at[s, group, pl.ds(al(me_y, len_i), len_i)],
                                 in_send.at[r, 0], in_recv.at[r, 0], 'mode1', q))
        for o in offsets_x:
            p = peer_x(o)
            x_list.append(remote(v.at[group, pl.ds(al(p, blk_i), blk_i)], lx.at[s, group, :, pl.ds(al(me_x, len_j), len_j), :],
                                 in_send.at[r, 1], in_recv.at[r, 1], 'mode2', p))
        core = remote(v.at[group], lc.at[s, group], in_send.at[r, 2], in_recv.at[r, 2 + s], 'mode3', other)
        return y_list, x_list, core

    def send_in(s, v, r):
        y_list, x_list, core = in_copies(s, v, r, order_y, order_x)
        for pair in zip(x_list, y_list):
            for copy in pair:
                copy.start()
        core.start()

    def wait_exchange(send, recv, y_span, x_span, r):
        for n, (axis, peer, span) in enumerate((('mode1', peer_y(1), y_span), ('mode2', peer_x(1), x_span))):
            copies = remote(span, span, send.at[r, n], recv.at[r, n], axis, peer)
            copies.wait_send()
            copies.wait_recv()

    def wait_in(s, r):
        group = pl.ds(r * PER, PER)
        wait_exchange(in_send, in_recv, ly.at[s, group, pl.ds(0, (n1 - 1) * len_i)], lx.at[s, group, :, pl.ds(0, (n2 - 1) * len_j), :], r)

    def out_x_copies(s, r, slot, last=False, offsets=all_x):
        copies = []
        home = tx_last if last else tx.at[s, pl.ds(r * PER, PER)]
        for o in offsets:
            p = peer_x(o)
            copies.append(remote(out_x.at[s % banks, slot, :, :, pl.ds(al(p, len_j), len_j), :], home.at[:, pl.ds(al(me_x, blk_i), blk_i)],
                                 out_send.at[r, 1], out_recv.at[r, 1], 'mode2', p))
        if last:
            return copies, None
        own = pltpu.make_async_copy(out_x.at[s % banks, slot, :, :, pl.ds(al(me_x, len_j), len_j), :],
                                    home.at[:, pl.ds(al(me_x, blk_i), blk_i)], own_sem.at[slot, 1])
        return copies, own

    def out_y_copies(s, r, slot, last=False, offsets=all_y):
        copies = []
        home = ty_last if last else ty.at[s, pl.ds(r * PER, PER)]
        for o in offsets:
            q = peer_y(o)
            copies.append(remote(out_y.at[s % banks, slot, :, pl.ds(al(q, len_i), len_i)], home.at[:, :, pl.ds(al(me_y, blk_j), blk_j), :],
                                 out_send.at[r, 0], out_recv.at[r, 0], 'mode1', q))
        if last:
            return copies, None
        own = pltpu.make_async_copy(out_y.at[s % banks, slot, :, pl.ds(al(me_y, len_i), len_i)],
                                    home.at[:, :, pl.ds(al(me_y, blk_j), blk_j), :], own_sem.at[slot, 0])
        return copies, own

    def products(s, v, r, last=False):
        slot = lax.rem(r, SLOTS)
        wait_in(s, r)
        blocks = buf_y.shape[1] // blk_j

        def loads_of(c):
            t, half = r * PER + c, lax.rem(c, 2)
            first, second = [], []
            for o in range(n2):
                p = peer_x(o)
                src = v.at[t, pl.ds(al(me_x, blk_i), blk_i)] if o == 0 else lx.at[s, t, :, pl.ds(al(p, len_j), len_j), :]
                first.append(pltpu.make_async_copy(src, buf_x.at[half, :, pl.ds(al(p, len_j), len_j), :], ld.at[half, 0]))
            for o in range(n1):
                q = peer_y(o)
                src = v.at[t, :, pl.ds(al(me_y, blk_j), blk_j), :] if o == 0 else ly.at[s, t, pl.ds(al(q, len_i), len_i)]
                second.append(pltpu.make_async_copy(src, buf_y.at[half, pl.ds(al(q, len_i), len_i)], ld.at[half, 1]))
            return first, second

        def start_loads(c):
            first, second = loads_of(c)
            for copy in first + second:
                copy.start()

        start_loads(0)

        @pl.loop(0, PER)
        def _(c):
            half = lax.rem(c, 2)

            @pl.when(c + 1 < PER)
            def _():
                start_loads(c + 1)

            pltpu.make_async_copy(buf_x.at[half], buf_x.at[half], ld.at[half, 0]).wait()

            @pl.loop(0, blk_i)
            def _(i):
                out_x[s % banks, slot, c, i] = jnp.dot(f2[s], buf_x[half, i], preferred_element_type=F32).astype(BF16)

            pltpu.make_async_copy(buf_y.at[half], buf_y.at[half], ld.at[half, 1]).wait()

            @pl.loop(0, blocks)
            def _(b):
                rows = pl.ds(al(b, blk_j), blk_j)
                mid_a[:, rows, :] = jnp.swapaxes(buf_y[half, rows], 0, 1)

            @pl.loop(0, blk_j)
            def _(j):
                mid_b[j] = jnp.dot(f1[s], mid_a[j], preferred_element_type=F32).astype(BF16)

            @pl.loop(0, blocks)
            def _(b):
                rows = pl.ds(al(b, blk_j), blk_j)
                out_y[s % banks, slot, c, rows] = jnp.swapaxes(mid_b[:, rows, :], 0, 1)

        copies_x, own_x = out_x_copies(s, r, slot, last, order_x)
        copies_y, own_y = out_y_copies(s, r, slot, last, order_y)
        for pair in zip(copies_x, copies_y):
            for copy in pair:
                copy.start()
        if last:
            tx_last[:, pl.ds(al(me_x, blk_i), blk_i)] = out_x[s % banks, slot, :, :, pl.ds(al(me_x, len_j), len_j), :]
            ty_last[:, :, pl.ds(al(me_y, blk_j), blk_j), :] = out_y[s % banks, slot, :, pl.ds(al(me_y, len_i), len_i)]
        else:
            own_x.start()
            own_y.start()

    step = max(1, 256 // len_j)
    flat = (step * len_j, len_k)

    def wait_core(s, v, r):
        core = in_copies(s, v, r)[2]
        core.wait_send()
        core.wait_recv()

    def wait_out(s, r, last=False):
        group = pl.ds(0, PER) if last else pl.ds(r * PER, PER)
        y_home, x_home = (ty_last, tx_last) if last else (ty.at[s], tx.at[s])
        wait_exchange(out_send, out_recv, y_home.at[group, :, pl.ds(0, (n1 - 1) * blk_j), :], x_home.at[group, pl.ds(0, (n2 - 1) * blk_i)], r)
        if not last:
            slot = lax.rem(r, SLOTS)
            out_x_copies(s, r, slot)[1].wait()
            out_y_copies(s, r, slot)[1].wait()

    def mode3(s, half, rows):
        return (jnp.dot(vb[half, rows].reshape(flat), g[s, 0], preferred_element_type=F32)
                + jnp.dot(cb[half, rows].reshape(flat), g[s, 1], preferred_element_type=F32)).astype(BF16)

    def store_w(t):
        return pltpu.make_async_copy(ws, w.at[t], w_sem)

    def combine(s, v, r):
        wait_core(s, v, r)
        wait_out(s, r)

        def loads_of(c):
            t, half = r * PER + c, lax.rem(c, 2)
            return [pltpu.make_async_copy(src, dst.at[half], ld.at[half, n]) for n, (src, dst) in enumerate(
                ((v.at[t], vb), (lc.at[s, t], cb), (ty.at[s, t], yb), (tx.at[s, t], xb)))]

        for copy in loads_of(0):
            copy.start()

        @pl.loop(0, PER)
        def _(c):
            t, half = r * PER + c, lax.rem(c, 2)

            @pl.when(c + 1 < PER)
            def _():
                for copy in loads_of(c + 1):
                    copy.start()

            for copy in loads_of(c):
                copy.wait()
            if s == 0:
                @pl.when(c > 0)
                def _():
                    store_w(t - 1).wait()

            @pl.loop(0, len_i // step)
            def _(b):
                rows = pl.ds(b * step, step)
                total = (yb[half, rows].reshape(flat).astype(F32) + xb[half, rows].reshape(flat).astype(F32)) + mode3(s, half, rows).astype(F32)
                if s == 0:
                    scaled = dv[rows].reshape(flat) * total.astype(BF16).astype(F32)
                    ws[rows] = scaled.astype(BF16).reshape(step, len_j, len_k)
                else:
                    z[t, rows] = total.reshape(step, len_j, len_k)

            if s == 0:
                store_w(t).start()

        if s == 0:
            store_w(r * PER + PER - 1).wait()

    barrier = pltpu.get_barrier_semaphore()
    for o in range(1, n1):
        pl.semaphore_signal(barrier, inc=1, device_id={'mode1': peer_y(o)}, device_id_type=pl.DeviceIdType.MESH)
    for o in range(1, n2):
        pl.semaphore_signal(barrier, inc=1, device_id={'mode2': peer_x(o)}, device_id_type=pl.DeviceIdType.MESH)
    pl.semaphore_signal(barrier, inc=1, device_id={'mode3': other}, device_id_type=pl.DeviceIdType.MESH)
    pl.semaphore_wait(barrier, n1 + n2 - 1)

    for r in range(AHEAD):
        send_in(0, x, r)

    mine, theirs = pl.ds(al(me_c, len_k), len_k), pl.ds(al(other, len_k), len_k)
    loads = [pltpu.make_async_copy(src, dst, w_sem if n == 8 else ld.at[n // 4, n % 4]) for n, (src, dst) in enumerate((
        (a1, f1.at[0]), (b1, f1.at[1]), (a2, f2.at[0]), (b2, f2.at[1]), (d, dv),
        (a3.at[mine, mine], g.at[0, 0]), (a3.at[mine, theirs], g.at[0, 1]),
        (b3.at[mine, mine], g.at[1, 0]), (b3.at[mine, theirs], g.at[1, 1])))]
    for copy in loads:
        copy.start()
    for copy in loads:
        copy.wait()
    for s in range(2):
        for c in range(2):
            g[s, c] = g[s, c].astype(F32).T.astype(BF16)

    @pl.loop(0, chunks + 1)
    def _(n):
        @pl.when(n < chunks)
        def _():
            products(0, x, n)

        @pl.when(n + AHEAD < chunks)
        def _():
            send_in(0, x, n + AHEAD)

        @pl.when(n >= 1)
        def _():
            combine(0, x, n - 1)
            send_in(1, w, n - 1)

        @pl.when(n >= 2)
        def _():
            products(1, w, n - 2)

        @pl.when(n >= 3)
        def _():
            combine(1, w, n - 3)

    last = chunks - 1
    products(1, w, last, True)
    combine(1, w, last - 1)
    wait_core(1, w, last)

    def last_loads(c):
        t, half = last * PER + c, lax.rem(c, 2)
        return [pltpu.make_async_copy(w.at[t], vb.at[half], ld.at[half, 0]), pltpu.make_async_copy(lc.at[1, t], cb.at[half], ld.at[half, 1])]

    for copy in last_loads(0):
        copy.start()

    @pl.loop(0, PER)
    def _(c):
        half = lax.rem(c, 2)

        @pl.when(c + 1 < PER)
        def _():
            for copy in last_loads(c + 1):
                copy.start()

        for copy in last_loads(c):
            copy.wait()

        @pl.loop(0, len_i // step)
        def _(b):
            rows = pl.ds(b * step, step)
            third_last[c, rows] = mode3(1, half, rows).reshape(step, len_j, len_k)

    wait_out(1, last, True)


def finish(z_first, third, ty, tx, z, zb, sem):
    done, len_i = z_first.shape[0], z_first.shape[1]
    for r in range(done):
        pltpu.make_async_copy(z_first.at[r], z.at[r], sem).start()
    for c in range(third.shape[0]):
        @pl.loop(0, len_i)
        def _(i):
            zb[c, i] = (ty[c, i].astype(F32) + tx[c, i].astype(F32)) + third[c, i].astype(F32)

        pltpu.make_async_copy(zb.at[c], z.at[done + c], sem).start()
    pltpu.make_async_copy(z, z, sem).wait()


def solution(mesh):
    n1, n2, n3 = mesh.shape['mode1'], mesh.shape['mode2'], mesh.shape['mode3']
    vol_spec = P('rhs', 'mode1', 'mode2', 'mode3')
    diag_spec = P('mode1', 'mode2', 'mode3')

    def local_op(x_vol, diag_vals, a1, a2, a3, b1, b2, b3):
        rhs, len_i, len_j, len_k = x_vol.shape
        m1, m2 = len_i * n1, len_j * n2
        blk_j, blk_i = len_j // n1, len_i // n2
        banks = 1 if rhs // PER <= SLOTS else 2
        any_spec = pl.BlockSpec(memory_space=pl.ANY)
        vmem_spec = pl.BlockSpec(memory_space=pltpu.VMEM)
        outs = [
            pltpu.VMEM((rhs - PER, len_i, len_j, len_k), F32),
            *[pltpu.VMEM((PER, len_i, len_j, len_k), BF16)] * 3,
            jax.ShapeDtypeStruct((rhs, len_i, len_j, len_k), BF16),
            jax.ShapeDtypeStruct((2, rhs, m1, blk_j, len_k), BF16),
            jax.ShapeDtypeStruct((2, rhs, blk_i, m2, len_k), BF16),
            jax.ShapeDtypeStruct((2, rhs, len_i, len_j, len_k), BF16),
            jax.ShapeDtypeStruct((2, rhs, len_i, len_j, len_k), BF16),
            jax.ShapeDtypeStruct((2, rhs, len_i, len_j, len_k), BF16),
        ]
        vmem, dma = pltpu.VMEM, pltpu.SemaphoreType.DMA
        local = (len_i, len_j, len_k)
        res = pl.pallas_call(
            functools.partial(kernel, n1, n2),
            out_shape=outs,
            in_specs=[any_spec] * 8,
            out_specs=[vmem_spec] * 4 + [any_spec] * (len(outs) - 4),
            scratch_shapes=[
                vmem((2, m1, m1), BF16), vmem((2, m2, m2), BF16), vmem((2, 2, len_k, len_k), BF16), vmem(local, F32),
                vmem((2, m1, blk_j, len_k), BF16), vmem((2, blk_i, m2, len_k), BF16),
                vmem((blk_j, m1, len_k), BF16), vmem((blk_j, m1, len_k), BF16),
                vmem((banks, SLOTS, PER, m1, blk_j, len_k), BF16), vmem((banks, SLOTS, PER, blk_i, m2, len_k), BF16),
                *[vmem((2, *local), BF16)] * 4,
                vmem(local, BF16),
                dma((rhs // PER, 3)), dma((rhs // PER, 4)), dma((rhs // PER, 2)), dma((rhs // PER, 2)),
                dma((SLOTS, 2)), dma((2, 4)), dma,
            ],
            compiler_params=pltpu.CompilerParams(collective_id=0, has_side_effects=True, vmem_limit_bytes=42 * 1024 * 1024),
            name='kron',
        )(x_vol, diag_vals, a1, a2, a3, b1, b2, b3)
        return pl.pallas_call(
            finish,
            out_shape=jax.ShapeDtypeStruct(x_vol.shape, F32),
            in_specs=[vmem_spec] * 4,
            out_specs=any_spec,
            scratch_shapes=[vmem((PER, *local), F32), dma],
            compiler_params=pltpu.CompilerParams(vmem_limit_bytes=12 * 1024 * 1024),
            name='finish',
        )(*res[:4])

    return jax.shard_map(local_op, mesh=mesh, in_specs=(vol_spec, diag_spec, P(), P(), P(), P(), P(), P()), out_specs=vol_spec, check_vma=False)
```

```python
import functools

import jax
import jax.numpy as jnp
from jax import lax
from jax.experimental import pallas as pl
from jax.experimental.pallas import tpu as pltpu
from jax.sharding import PartitionSpec as P

BF16, F32 = jnp.bfloat16, jnp.float32
AHEAD = 2
SLOTS = 2
PER = 4


def kernel(n1, n2, x, d, a1, a2, a3, b1, b2, b3, z, third_last, ty_last, tx_last, w, ly, lx, lc, ty, tx,
           f1, f2, g, dv, buf_y, buf_x, mid_a, mid_b, out_y, out_x, vb, cb, yb, xb, ws,
           send_sem, in_recv, out_recv, own_sem, ld, w_sem):
    rhs, len_i, len_j, len_k = x.shape
    blk_j, blk_i = len_j // n1, len_i // n2
    me_y, me_x, me_c = lax.axis_index('mode1'), lax.axis_index('mode2'), lax.axis_index('mode3')
    other = 1 - me_c
    chunks = rhs // PER
    banks = out_y.shape[0]

    def send_order(n):
        near_first, far_first = (1, n - 1, *range(2, n - 1)), (*range(2, n - 1), 1, n - 1)
        return [a + me_c * (b - a) for a, b in zip(near_first, far_first)]

    order_y, order_x = send_order(n1), send_order(n2)
    all_y, all_x = range(1, n1), range(1, n2)

    def peer_y(o):
        return lax.rem(me_y + o, n1)

    def peer_x(o):
        return lax.rem(me_x + o, n2)

    def al(v, m):
        return pl.multiple_of(v * m, m)

    def remote(src, dst, send, recv, axis, index):
        return pltpu.make_async_remote_copy(src_ref=src, dst_ref=dst, send_sem=send, recv_sem=recv,
                                            device_id={axis: index}, device_id_type=pl.DeviceIdType.MESH)

    def in_copies(s, v, r, offsets_y=all_y, offsets_x=all_x):
        y_list, x_list = [], []
        group = pl.ds(r * PER, PER)
        for o in offsets_y:
            q = peer_y(o)
            y_list.append(remote(v.at[group, :, pl.ds(al(q, blk_j), blk_j), :], ly.at[s, group, pl.ds(al(me_y, len_i), len_i)],
                                 send_sem.at[r, 0], in_recv.at[r, 0], 'mode1', q))
        for o in offsets_x:
            p = peer_x(o)
            x_list.append(remote(v.at[group, pl.ds(al(p, blk_i), blk_i)], lx.at[s, group, :, pl.ds(al(me_x, len_j), len_j), :],
                                 send_sem.at[r, 1], in_recv.at[r, 1], 'mode2', p))
        core = remote(v.at[group], lc.at[s, group], send_sem.at[r, 2], in_recv.at[r, 2 + s], 'mode3', other)
        return y_list, x_list, core

    def send_in(s, v, r):
        y_list, x_list, core = in_copies(s, v, r, order_y, order_x)
        for pair in zip(x_list, y_list):
            for copy in pair:
                copy.start()
        core.start()

    def wait_exchange(send, recv, y_span, x_span, r):
        for n, (axis, peer, span) in enumerate((('mode1', peer_y(1), y_span), ('mode2', peer_x(1), x_span))):
            copies = remote(span, span, send.at[r, n], recv.at[r, n], axis, peer)
            copies.wait_send()
            copies.wait_recv()

    def wait_in(s, r):
        group = pl.ds(r * PER, PER)
        wait_exchange(send_sem, in_recv, ly.at[s, group, pl.ds(0, (n1 - 1) * len_i)], lx.at[s, group, :, pl.ds(0, (n2 - 1) * len_j), :], r)

    def out_x_copies(s, r, slot, last=False, offsets=all_x):
        copies = []
        home = tx_last if last else tx.at[s, pl.ds(r * PER, PER)]
        for o in offsets:
            p = peer_x(o)
            copies.append(remote(out_x.at[s % banks, slot, :, :, pl.ds(al(p, len_j), len_j), :], home.at[:, pl.ds(al(me_x, blk_i), blk_i)],
                                 send_sem.at[r, 1], out_recv.at[r, 1], 'mode2', p))
        if last:
            return copies, None
        own = pltpu.make_async_copy(out_x.at[s % banks, slot, :, :, pl.ds(al(me_x, len_j), len_j), :],
                                    home.at[:, pl.ds(al(me_x, blk_i), blk_i)], own_sem.at[slot, 1])
        return copies, own

    def out_y_copies(s, r, slot, last=False, offsets=all_y):
        copies = []
        home = ty_last if last else ty.at[s, pl.ds(r * PER, PER)]
        for o in offsets:
            q = peer_y(o)
            copies.append(remote(out_y.at[s % banks, slot, :, pl.ds(al(q, len_i), len_i)], home.at[:, :, pl.ds(al(me_y, blk_j), blk_j), :],
                                 send_sem.at[r, 0], out_recv.at[r, 0], 'mode1', q))
        if last:
            return copies, None
        own = pltpu.make_async_copy(out_y.at[s % banks, slot, :, pl.ds(al(me_y, len_i), len_i)],
                                    home.at[:, :, pl.ds(al(me_y, blk_j), blk_j), :], own_sem.at[slot, 0])
        return copies, own

    def products(s, v, r, last=False):
        slot = lax.rem(r, SLOTS)
        wait_in(s, r)
        blocks = buf_y.shape[1] // blk_j

        def loads_of(c):
            t, half = r * PER + c, lax.rem(c, 2)
            first, second = [], []
            for o in range(n2):
                p = peer_x(o)
                src = v.at[t, pl.ds(al(me_x, blk_i), blk_i)] if o == 0 else lx.at[s, t, :, pl.ds(al(p, len_j), len_j), :]
                first.append(pltpu.make_async_copy(src, buf_x.at[half, :, pl.ds(al(p, len_j), len_j), :], ld.at[half, 0]))
            for o in range(n1):
                q = peer_y(o)
                src = v.at[t, :, pl.ds(al(me_y, blk_j), blk_j), :] if o == 0 else ly.at[s, t, pl.ds(al(q, len_i), len_i)]
                second.append(pltpu.make_async_copy(src, buf_y.at[half, pl.ds(al(q, len_i), len_i)], ld.at[half, 1]))
            return first, second

        def start_loads(c):
            first, second = loads_of(c)
            for copy in first + second:
                copy.start()

        start_loads(0)

        @pl.loop(0, PER)
        def _(c):
            half = lax.rem(c, 2)

            @pl.when(c + 1 < PER)
            def _():
                start_loads(c + 1)

            pltpu.make_async_copy(buf_x.at[half], buf_x.at[half], ld.at[half, 0]).wait()

            @pl.loop(0, blk_i)
            def _(i):
                out_x[s % banks, slot, c, i] = jnp.dot(f2[s], buf_x[half, i], preferred_element_type=F32).astype(BF16)

            pltpu.make_async_copy(buf_y.at[half], buf_y.at[half], ld.at[half, 1]).wait()

            @pl.loop(0, blocks)
            def _(b):
                rows = pl.ds(al(b, blk_j), blk_j)
                mid_a[:, rows, :] = jnp.swapaxes(buf_y[half, rows], 0, 1)

            @pl.loop(0, blk_j)
            def _(j):
                mid_b[j] = jnp.dot(f1[s], mid_a[j], preferred_element_type=F32).astype(BF16)

            @pl.loop(0, blocks)
            def _(b):
                rows = pl.ds(al(b, blk_j), blk_j)
                out_y[s % banks, slot, c, rows] = jnp.swapaxes(mid_b[:, rows, :], 0, 1)

        copies_x, own_x = out_x_copies(s, r, slot, last, order_x)
        copies_y, own_y = out_y_copies(s, r, slot, last, order_y)
        for pair in zip(copies_x, copies_y):
            for copy in pair:
                copy.start()
        if last:
            tx_last[:, pl.ds(al(me_x, blk_i), blk_i)] = out_x[s % banks, slot, :, :, pl.ds(al(me_x, len_j), len_j), :]
            ty_last[:, :, pl.ds(al(me_y, blk_j), blk_j), :] = out_y[s % banks, slot, :, pl.ds(al(me_y, len_i), len_i)]
        else:
            own_x.start()
            own_y.start()

    step = max(1, 256 // len_j)
    flat = (step * len_j, len_k)

    def wait_core(s, v, r):
        core = in_copies(s, v, r)[2]
        core.wait_send()
        core.wait_recv()

    def wait_out(s, r, last=False):
        group = pl.ds(0, PER) if last else pl.ds(r * PER, PER)
        y_home, x_home = (ty_last, tx_last) if last else (ty.at[s], tx.at[s])
        wait_exchange(send_sem, out_recv, y_home.at[group, :, pl.ds(0, (n1 - 1) * blk_j), :], x_home.at[group, pl.ds(0, (n2 - 1) * blk_i)], r)
        if not last:
            slot = lax.rem(r, SLOTS)
            out_x_copies(s, r, slot)[1].wait()
            out_y_copies(s, r, slot)[1].wait()

    def mode3(s, half, rows):
        return (jnp.dot(vb[half, rows].reshape(flat), g[s, 0], preferred_element_type=F32)
                + jnp.dot(cb[half, rows].reshape(flat), g[s, 1], preferred_element_type=F32)).astype(BF16)

    def store_w(t):
        return pltpu.make_async_copy(ws, w.at[t], w_sem)

    def combine(s, v, r):
        wait_core(s, v, r)
        wait_out(s, r)

        def loads_of(c):
            t, half = r * PER + c, lax.rem(c, 2)
            return [pltpu.make_async_copy(src, dst.at[half], ld.at[half, n]) for n, (src, dst) in enumerate(
                ((v.at[t], vb), (lc.at[s, t], cb), (ty.at[s, t], yb), (tx.at[s, t], xb)))]

        for copy in loads_of(0):
            copy.start()

        @pl.loop(0, PER)
        def _(c):
            t, half = r * PER + c, lax.rem(c, 2)

            @pl.when(c + 1 < PER)
            def _():
                for copy in loads_of(c + 1):
                    copy.start()

            for copy in loads_of(c):
                copy.wait()
            if s == 0:
                @pl.when(c > 0)
                def _():
                    store_w(t - 1).wait()

            @pl.loop(0, len_i // step)
            def _(b):
                rows = pl.ds(b * step, step)
                total = (yb[half, rows].reshape(flat).astype(F32) + xb[half, rows].reshape(flat).astype(F32)) + mode3(s, half, rows).astype(F32)
                if s == 0:
                    scaled = dv[rows].reshape(flat) * total.astype(BF16).astype(F32)
                    ws[rows] = scaled.astype(BF16).reshape(step, len_j, len_k)
                else:
                    z[t, rows] = total.reshape(step, len_j, len_k)

            if s == 0:
                store_w(t).start()

        if s == 0:
            store_w(r * PER + PER - 1).wait()

    barrier = pltpu.get_barrier_semaphore()
    for o in range(1, n1):
        pl.semaphore_signal(barrier, inc=1, device_id={'mode1': peer_y(o)}, device_id_type=pl.DeviceIdType.MESH)
    for o in range(1, n2):
        pl.semaphore_signal(barrier, inc=1, device_id={'mode2': peer_x(o)}, device_id_type=pl.DeviceIdType.MESH)
    pl.semaphore_signal(barrier, inc=1, device_id={'mode3': other}, device_id_type=pl.DeviceIdType.MESH)
    pl.semaphore_wait(barrier, n1 + n2 - 1)

    for r in range(AHEAD):
        send_in(0, x, r)

    mine, theirs = pl.ds(al(me_c, len_k), len_k), pl.ds(al(other, len_k), len_k)
    loads = [pltpu.make_async_copy(src, dst, w_sem if n == 8 else ld.at[n // 4, n % 4]) for n, (src, dst) in enumerate((
        (a1, f1.at[0]), (b1, f1.at[1]), (a2, f2.at[0]), (b2, f2.at[1]), (d, dv),
        (a3.at[mine, mine], g.at[0, 0]), (a3.at[mine, theirs], g.at[0, 1]),
        (b3.at[mine, mine], g.at[1, 0]), (b3.at[mine, theirs], g.at[1, 1])))]
    for copy in loads:
        copy.start()
    for copy in loads:
        copy.wait()
    for s in range(2):
        for c in range(2):
            g[s, c] = g[s, c].astype(F32).T.astype(BF16)

    @pl.loop(0, chunks + 1)
    def _(n):
        @pl.when(n < chunks)
        def _():
            products(0, x, n)

        @pl.when(n + AHEAD < chunks)
        def _():
            send_in(0, x, n + AHEAD)

        @pl.when(n >= 1)
        def _():
            combine(0, x, n - 1)
            send_in(1, w, n - 1)

        @pl.when(n >= 2)
        def _():
            products(1, w, n - 2)

        @pl.when(n >= 3)
        def _():
            combine(1, w, n - 3)

    last = chunks - 1
    products(1, w, last, True)
    combine(1, w, last - 1)
    wait_core(1, w, last)

    def last_loads(c):
        t, half = last * PER + c, lax.rem(c, 2)
        return [pltpu.make_async_copy(w.at[t], vb.at[half], ld.at[half, 0]), pltpu.make_async_copy(lc.at[1, t], cb.at[half], ld.at[half, 1])]

    for copy in last_loads(0):
        copy.start()

    @pl.loop(0, PER)
    def _(c):
        half = lax.rem(c, 2)

        @pl.when(c + 1 < PER)
        def _():
            for copy in last_loads(c + 1):
                copy.start()

        for copy in last_loads(c):
            copy.wait()

        @pl.loop(0, len_i // step)
        def _(b):
            rows = pl.ds(b * step, step)
            third_last[c, rows] = mode3(1, half, rows).reshape(step, len_j, len_k)

    wait_out(1, last, True)


def finish(z_first, third, ty, tx, z, zb, sem):
    done, len_i = z_first.shape[0], z_first.shape[1]
    for r in range(done):
        pltpu.make_async_copy(z_first.at[r], z.at[r], sem).start()
    for c in range(third.shape[0]):
        @pl.loop(0, len_i)
        def _(i):
            zb[c, i] = (ty[c, i].astype(F32) + tx[c, i].astype(F32)) + third[c, i].astype(F32)

        pltpu.make_async_copy(zb.at[c], z.at[done + c], sem).start()
    pltpu.make_async_copy(z, z, sem).wait()


def solution(mesh):
    n1, n2, n3 = mesh.shape['mode1'], mesh.shape['mode2'], mesh.shape['mode3']
    vol_spec = P('rhs', 'mode1', 'mode2', 'mode3')
    diag_spec = P('mode1', 'mode2', 'mode3')

    def local_op(x_vol, diag_vals, a1, a2, a3, b1, b2, b3):
        rhs, len_i, len_j, len_k = x_vol.shape
        m1, m2 = len_i * n1, len_j * n2
        blk_j, blk_i = len_j // n1, len_i // n2
        banks = 1 if rhs // PER <= SLOTS else 2
        any_spec = pl.BlockSpec(memory_space=pl.ANY)
        vmem_spec = pl.BlockSpec(memory_space=pltpu.VMEM)
        outs = [
            pltpu.VMEM((rhs - PER, len_i, len_j, len_k), F32),
            *[pltpu.VMEM((PER, len_i, len_j, len_k), BF16)] * 3,
            jax.ShapeDtypeStruct((rhs, len_i, len_j, len_k), BF16),
            jax.ShapeDtypeStruct((2, rhs, m1, blk_j, len_k), BF16),
            jax.ShapeDtypeStruct((2, rhs, blk_i, m2, len_k), BF16),
            jax.ShapeDtypeStruct((2, rhs, len_i, len_j, len_k), BF16),
            jax.ShapeDtypeStruct((2, rhs, len_i, len_j, len_k), BF16),
            jax.ShapeDtypeStruct((2, rhs, len_i, len_j, len_k), BF16),
        ]
        vmem, dma = pltpu.VMEM, pltpu.SemaphoreType.DMA
        local = (len_i, len_j, len_k)
        res = pl.pallas_call(
            functools.partial(kernel, n1, n2),
            out_shape=outs,
            in_specs=[any_spec] * 8,
            out_specs=[vmem_spec] * 4 + [any_spec] * (len(outs) - 4),
            scratch_shapes=[
                vmem((2, m1, m1), BF16), vmem((2, m2, m2), BF16), vmem((2, 2, len_k, len_k), BF16), vmem(local, F32),
                vmem((2, m1, blk_j, len_k), BF16), vmem((2, blk_i, m2, len_k), BF16),
                vmem((blk_j, m1, len_k), BF16), vmem((blk_j, m1, len_k), BF16),
                vmem((banks, SLOTS, PER, m1, blk_j, len_k), BF16), vmem((banks, SLOTS, PER, blk_i, m2, len_k), BF16),
                *[vmem((2, *local), BF16)] * 4,
                vmem(local, BF16),
                dma((rhs // PER, 3)), dma((rhs // PER, 4)), dma((rhs // PER, 2)),
                dma((SLOTS, 2)), dma((2, 4)), dma,
            ],
            compiler_params=pltpu.CompilerParams(collective_id=0, has_side_effects=True, vmem_limit_bytes=42 * 1024 * 1024),
            name='kron',
        )(x_vol, diag_vals, a1, a2, a3, b1, b2, b3)
        return pl.pallas_call(
            finish,
            out_shape=jax.ShapeDtypeStruct(x_vol.shape, F32),
            in_specs=[vmem_spec] * 4,
            out_specs=any_spec,
            scratch_shapes=[vmem((PER, *local), F32), dma],
            compiler_params=pltpu.CompilerParams(vmem_limit_bytes=12 * 1024 * 1024),
            name='finish',
        )(*res[:4])

    return jax.shard_map(local_op, mesh=mesh, in_specs=(vol_spec, diag_spec, P(), P(), P(), P(), P(), P()), out_specs=vol_spec, check_vma=False)
```
